16 devices in a mesh: dp: 4 (over y, z, core), tp: 4 (over x).
Axes of the slice: x: 4, y: 2, z: 1, core: 2. Of those that a mesh axis runs over, the one named last changes fastest.
The devices are a block of a 4x4x8 slice.
Arguments:
- x: bfloat16 [8192, 6144], P('dp'), parts along dimension 0
- gain: bfloat16 [6144], replicated
- wq: bfloat16 [6144, 6144], P(None, 'tp')
- wk: bfloat16 [6144, 1024], P(None, 'tp')
- wv: bfloat16 [6144, 1024], P(None, 'tp')
- wo: bfloat16 [6144, 6144], P('tp')
Outputs:
- output: bfloat16 [8192, 6144], P('dp'), parts along dimension 0
There are 4 independent parts. The reference program is written for one: setup_inputs(seed, part) draws one part's arguments, and reference() takes and returns one part's arrays. A program takes and returns all parts, laid end to end along the dimension named above; an argument that names none is the same for every part.
All inputs are finite; a program needn't handle non-finite values.
Results may differ from the reference program's by a relative error of at most 0.012.
Values are sent between devices in bfloat16 or wider.
A program may use at most 768 MiB of HBM per device.

```python
import jax
import jax.numpy as jnp
from jax import lax

ROWS = 2048
D = 6144
HEADS = 48
KV_HEADS = 8
HEAD = 128
THETA = 10000


def setup_inputs(seed: int = 0, part: int = 0) -> dict:
    kx, kn, kq, kk, kv, ko = jax.random.split(jax.random.key(seed), 6)

    def weights(key, rows, columns):
        return jax.random.normal(key, (rows, columns), jnp.float32) * rows**-0.5

    drawn = {
        "x": jax.random.normal(jax.random.fold_in(kx, part), (ROWS, D), jnp.float32),
        "gain": 1 + 0.1 * jax.random.normal(kn, (D,), jnp.float32),
        "wq": 2 * weights(kq, D, HEADS * HEAD),
        "wk": 2 * weights(kk, D, KV_HEADS * HEAD),
        "wv": 4 * weights(kv, D, KV_HEADS * HEAD),
        "wo": weights(ko, HEADS * HEAD, D),
    }
    return {k: v.astype(jnp.bfloat16) for k, v in drawn.items()}


def normed(x, gain):
    wide = x.astype(jnp.float32)
    scale = lax.rsqrt(jnp.mean(wide * wide, -1, keepdims=True) + 1e-6)
    return (wide * scale * gain.astype(jnp.float32)).astype(jnp.bfloat16)


def turned(t, place, theta):
    half = t.shape[-1] // 2
    angle = place.astype(jnp.float32)[:, None] * theta ** (-jnp.arange(half, dtype=jnp.float32) / half)
    cos, sin = jnp.cos(angle)[:, None], jnp.sin(angle)[:, None]
    a, b = t[..., :half].astype(jnp.float32), t[..., half:].astype(jnp.float32)
    return jnp.concatenate([a * cos - b * sin, b * cos + a * sin], -1).astype(jnp.bfloat16)


def matmul(a, w):
    return jnp.dot(a, w, preferred_element_type=jnp.float32).astype(jnp.bfloat16)


def einsum(form, a, b):
    return jnp.einsum(form, a.astype(jnp.float32), b.astype(jnp.float32))


def attention(q, k, v):
    scores = einsum("tgsd,ugd->gstu", q, k) * q.shape[-1] ** -0.5
    token = jnp.arange(q.shape[0])
    scores = jnp.where(token[:, None] >= token, scores, -jnp.inf)
    weights = jax.nn.softmax(scores, -1).astype(jnp.bfloat16)
    return einsum("gstu,ugd->tgsd", weights, v).astype(jnp.bfloat16)


def reference(x, gain, wq, wk, wv, wo):
    a, place = normed(x, gain), jnp.arange(ROWS)
    q = turned(matmul(a, wq).reshape(ROWS, HEADS, HEAD), place, THETA).reshape(ROWS, KV_HEADS, -1, HEAD)
    k = turned(matmul(a, wk).reshape(ROWS, KV_HEADS, HEAD), place, THETA)
    v = matmul(a, wv).reshape(ROWS, KV_HEADS, HEAD)
    seen = attention(q, k, v).reshape(ROWS, HEADS * HEAD)
    return (x.astype(jnp.float32) + jnp.dot(seen, wo, preferred_element_type=jnp.float32)).astype(jnp.bfloat16)
```

```python
import functools

import jax
import jax.numpy as jnp
from jax import lax
from jax.experimental import pallas as pl
from jax.experimental.pallas import tpu as pltpu
from jax.sharding import PartitionSpec as P

HEAD = 128
THETA = 10000
NEG = -1e30
HIDDEN = 2 * NEG
LOG2E = 1.4426950408889634
VMEM = 67_000_000
ROWS = 128
KEYS = 256
F32, BF16 = jnp.float32, jnp.bfloat16
OB, OA, RA, LB, RB, LA, YBR, YAR, YAL, YBL, FWR, FWL = range(12)


def _dot(a, b, ca, cb):
    return lax.dot_general(a, b, (((ca,), (cb,)), ((), ())), preferred_element_type=F32)


def _kernel(freq_ref, gain_ref, x_hbm, wq_hbm, wk_hbm, wv_hbm, wo_hbm, y_hbm,
            wq, wk, wv, wo, x_s, h_s, xown_s, cos_s, sin_s, q_s, k_s, vt_s, top_s, mix_s, seen_s,
            mid_s, own_s, term_s, pass_s, fin_s, got_s, far_s,
            w_sem, x_sem, y_sem, send_sem, recv_sem, *, n, axis):
    rows, d = x_hbm.shape
    chunks = rows // ROWS
    wide = wq.shape[1]
    kv = wk.shape[1] // HEAD
    g = wide // HEAD // kv
    part, half = d // n, d // n // 2
    cols = g * ROWS
    strip = cols // 2
    e = HEAD**-0.5 * LOG2E
    i = lax.axis_index(axis)
    r, l, o = lax.rem(i + 1, n), lax.rem(i + n - 1, n), lax.rem(i + 2, n)

    def column(owner, b):
        return pl.ds(pl.multiple_of(owner * part + b * half, 128), half)

    def row(c):
        return pl.ds(pl.multiple_of(c * ROWS, ROWS), ROWS)

    def remote(kind, c):
        s2, s4 = lax.rem(c, 2), lax.rem(c, 4)
        to = r if kind in (OB, RA, RB, YBR, YAR, FWR) else l
        if kind in (OB, OA):
            src, dst = term_s.at[s2, kind], got_s.at[s2, kind]
        elif kind in (RA, LB):
            src, dst = term_s.at[s2, kind], far_s.at[s4, kind - RA]
        elif kind in (RB, LA):
            src, dst = pass_s.at[s2, kind - RB], far_s.at[s4, kind - RA]
        elif kind in (YBR, YBL):
            src, dst = fin_s.at[s2, 1], y_hbm.at[row(c), column(i, 1)]
        elif kind in (YAR, YAL):
            src, dst = fin_s.at[s2, 0], y_hbm.at[row(c), column(i, 0)]
        elif kind == FWR:
            src = dst = y_hbm.at[row(c), column(l, 1)]
        else:
            src = dst = y_hbm.at[row(c), column(r, 0)]
        return pltpu.make_async_remote_copy(
            src_ref=src, dst_ref=dst, send_sem=send_sem.at[kind, s2], recv_sem=recv_sem.at[kind, s4],
            device_id={axis: to}, device_id_type=pl.DeviceIdType.MESH,
        )

    def local(c, b):
        s2 = lax.rem(c, 2)
        return pltpu.make_async_copy(fin_s.at[s2, b], y_hbm.at[row(c), column(i, b)], y_sem.at[b, s2])

    def chunk_in(c):
        return pltpu.make_async_copy(x_hbm.at[row(c), :], x_s, x_sem)

    tile = 256
    q_tiles = [pltpu.make_async_copy(wq_hbm.at[:, pl.ds(t * tile, tile)], wq.at[:, pl.ds(t * tile, tile)], w_sem.at[t]) for t in range(wide // tile)]
    k_in = pltpu.make_async_copy(wk_hbm, wk, w_sem.at[len(q_tiles)])
    v_in = pltpu.make_async_copy(wv_hbm, wv, w_sem.at[len(q_tiles) + 1])
    o_in = pltpu.make_async_copy(wo_hbm, wo, w_sem.at[len(q_tiles) + 2])

    chunk_in(0).start()
    k_in.start()
    v_in.start()
    for copy in q_tiles:
        copy.start()
    o_in.start()
    barrier = pltpu.get_barrier_semaphore()
    for to in (l, r):
        pl.semaphore_signal(barrier, inc=1, device_id={axis: to}, device_id_type=pl.DeviceIdType.MESH)

    k_s[...] = jnp.zeros(k_s.shape, BF16)
    for m in range(kv):
        vt_s[m, :HEAD, :] = jnp.zeros((HEAD, rows), BF16)
        vt_s[m, HEAD:, :] = jnp.ones((vt_s.shape[1] - HEAD, rows), BF16)
    pl.semaphore_wait(barrier, 2)

    def project(c):
        chunk_in(c).wait()

        def norm(t, _):
            at = pl.ds(pl.multiple_of(t * 16, 16), 16)
            w = x_s[at, :].astype(F32)
            scale = lax.rsqrt(jnp.mean(w * w, -1, keepdims=True) + 1e-6)
            h_s[at, :] = (w * scale * gain_ref[...].astype(F32)).astype(BF16)

        lax.fori_loop(0, ROWS // 16, norm, None)
        xown_s[...] = x_s[:, pl.ds(pl.multiple_of(i * part, 128), part)]

        @pl.when(c + 1 < chunks)
        def _():
            chunk_in(c + 1).start()

        place = lax.broadcasted_iota(jnp.int32, (ROWS, HEAD), 0) + c * ROWS
        angle = place.astype(F32) * freq_ref[...]
        sign = jnp.where(lax.broadcasted_iota(jnp.int32, (ROWS, HEAD), 1) < HEAD // 2, -1.0, 1.0)
        cos_s[...] = jnp.cos(angle)
        sin_s[...] = jnp.sin(angle) * sign

        def first(copy):
            @pl.when(c == 0)
            def _():
                copy.wait()

        def turned(t):
            t = t.astype(BF16).astype(F32)
            return (t * cos_s[...] + pltpu.roll(t, HEAD // 2, 1) * sin_s[...]).astype(BF16)

        first(k_in)
        t = _dot(h_s[...], wk[...], 1, 0)
        for m in range(kv):
            k_s[row(c), m * HEAD : (m + 1) * HEAD] = turned(t[:, m * HEAD : (m + 1) * HEAD])
        first(v_in)
        t = _dot(h_s[...], wv[...], 1, 0)
        for m in range(kv):
            vt_s[m, :HEAD, row(c)] = t[:, m * HEAD : (m + 1) * HEAD].T.astype(BF16)
        for p, copy in enumerate(q_tiles):
            first(copy)
            t = _dot(h_s[...], wq[:, p * tile : (p + 1) * tile], 1, 0)
            for m in range(tile // HEAD):
                head = p * (tile // HEAD) + m
                q_s[head // g, head % g * ROWS : (head % g + 1) * ROWS, :] = turned(t[:, m * HEAD : (m + 1) * HEAD])

    def attend(c):
        pieces = [(m, at) for m in range(kv) for at in range(0, cols, strip)]
        top_s[...] = jnp.full(top_s.shape, NEG, F32)
        mix_s[...] = jnp.zeros(mix_s.shape, F32)

        def block(j, masked):
            here = pl.ds(pl.multiple_of(j * KEYS, KEYS), KEYS)
            scores = [_dot(k_s[here, m * HEAD : (m + 1) * HEAD], q_s[m, at : at + strip, :], 1, 1) for m, at in pieces]
            if masked:
                query = lax.rem(lax.broadcasted_iota(jnp.int32, (KEYS, strip), 1), ROWS) + c * ROWS
                ok = query >= lax.broadcasted_iota(jnp.int32, (KEYS, strip), 0) + j * KEYS
            weights, keeps = [], []
            for (m, at), s in zip(pieces, scores):
                if masked:
                    s = jnp.where(ok, s, HIDDEN)
                old = top_s[m : m + 1, at : at + strip]
                top = jnp.maximum(old, s.max(axis=0, keepdims=True))
                top_s[m : m + 1, at : at + strip] = top
                weights.append(jnp.exp2((s - top) * e).astype(BF16))
                keeps.append(jnp.exp2((old - top) * e))
            for (m, at), p, keep in zip(pieces, weights, keeps):
                mix_s[m, :, at : at + strip] = mix_s[m, :, at : at + strip] * keep + _dot(vt_s[m, :, here], p, 1, 0)

        whole = lax.div(c * ROWS, KEYS)
        lax.fori_loop(0, whole, lambda j, _: block(j, False), None)
        block(whole, True)
        for m in range(kv):
            out = (mix_s[m, :HEAD, :] * (1 / mix_s[m, HEAD : HEAD + 1, :])).T.astype(BF16)
            for h in range(g):
                at = (m * g + h) * HEAD
                seen_s[:, at : at + HEAD] = out[h * ROWS : (h + 1) * ROWS, :]

    def terms(c):
        s2 = lax.rem(c, 2)

        @pl.when(c == 0)
        def _():
            o_in.wait()

        @pl.when(c >= 2)
        def _():
            for kind in (OB, OA, RA, LB):
                remote(kind, c - 2).wait_send()

        for kind, owner, b in ((OB, o, 1), (OA, o, 0), (RA, r, 0), (LB, l, 1)):
            term_s[s2, kind] = _dot(seen_s[...], wo[:, column(owner, b)], 1, 0).astype(BF16)
            remote(kind, c).start()
        mid_s[0] = _dot(seen_s[...], wo[:, column(r, 1)], 1, 0)
        mid_s[1] = _dot(seen_s[...], wo[:, column(l, 0)], 1, 0)
        for b in range(2):
            own_s[s2, b] = xown_s[:, b * half : (b + 1) * half].astype(F32) + _dot(seen_s[...], wo[:, column(i, b)], 1, 0)

    def pass_on(c):
        s2 = lax.rem(c, 2)

        @pl.when(c >= 2)
        def _():
            for kind in (RB, LA):
                remote(kind, c - 2).wait_send()

        for kind in (OB, OA):
            remote(kind, c).wait_recv()
            pass_s[s2, kind] = (mid_s[kind] + got_s[s2, kind].astype(F32)).astype(BF16)
        for kind in (RB, LA):
            remote(kind, c).start()

    def finish(c):
        s2, s4 = lax.rem(c, 2), lax.rem(c, 4)

        @pl.when(c >= 2)
        def _():
            for kind in (YBR, YAR, YAL, YBL):
                remote(kind, c - 2).wait_send()
            for b in range(2):
                local(c - 2, b).wait()

        for kind in (RA, LB, RB, LA):
            remote(kind, c).wait_recv()
        fin_s[s2, 1] = (own_s[s2, 1] + far_s[s4, LB - RA].astype(F32) + far_s[s4, RB - RA].astype(F32)).astype(BF16)
        fin_s[s2, 0] = (own_s[s2, 0] + far_s[s4, RA - RA].astype(F32) + far_s[s4, LA - RA].astype(F32)).astype(BF16)
        for kind in (YBR, YAL, YAR, YBL):
            remote(kind, c).start()
        for b in range(2):
            local(c, b).start()

    def forward(c):
        @pl.when(c >= 2)
        def _():
            for kind in (FWR, FWL):
                remote(kind, c - 2).wait_send()

        for kind, after in ((FWR, YBR), (FWL, YAL)):
            remote(after, c).wait_recv()
            remote(kind, c).start()

    def arrive(c):
        for kind in (YAR, YBL, FWR, FWL):
            remote(kind, c).wait_recv()

    def turn(c, _):
        def when(lag, do):
            @pl.when((c >= lag) & (c < chunks + lag))
            def _():
                do(c - lag)

        when(0, project)
        when(1, pass_on)
        when(0, attend)
        when(2, finish)
        when(0, terms)
        when(3, forward)
        when(4, arrive)

    lax.fori_loop(0, chunks + 5, turn, None)
    for c in (chunks - 2, chunks - 1):
        for kind in range(12):
            remote(kind, c).wait_send()
        for b in range(2):
            local(c, b).wait()


def layer(x, gain, freq, wq, wk, wv, wo, n, axis):
    rows, d = x.shape
    wide, kv = wq.shape[1], wk.shape[1] // HEAD
    g = wide // HEAD // kv
    half = d // n // 2
    cols = g * ROWS
    vmem, hbm = pl.BlockSpec(memory_space=pltpu.VMEM), pl.BlockSpec(memory_space=pl.ANY)
    return pl.pallas_call(
        functools.partial(_kernel, n=n, axis=axis),
        in_specs=[vmem, vmem] + [hbm] * 5,
        out_specs=hbm,
        out_shape=jax.ShapeDtypeStruct((rows, d), BF16),
        scratch_shapes=[
            pltpu.VMEM(wq.shape, BF16),
            pltpu.VMEM(wk.shape, BF16),
            pltpu.VMEM(wv.shape, BF16),
            pltpu.VMEM(wo.shape, BF16),
            pltpu.VMEM((ROWS, d), BF16),
            pltpu.VMEM((ROWS, d), BF16),
            pltpu.VMEM((ROWS, d // n), BF16),
            pltpu.VMEM((ROWS, HEAD), F32),
            pltpu.VMEM((ROWS, HEAD), F32),
            pltpu.VMEM((kv, cols, HEAD), BF16),
            pltpu.VMEM((rows, kv * HEAD), BF16),
            pltpu.VMEM((kv, HEAD + 16, rows), BF16),
            pltpu.VMEM((kv, cols), F32),
            pltpu.VMEM((kv, HEAD + 16, cols), F32),
            pltpu.VMEM((ROWS, wide), BF16),
            pltpu.VMEM((2, ROWS, half), F32),
            pltpu.VMEM((2, 2, ROWS, half), F32),
            pltpu.VMEM((2, 4, ROWS, half), BF16),
            pltpu.VMEM((2, 2, ROWS, half), BF16),
            pltpu.VMEM((2, 2, ROWS, half), BF16),
            pltpu.VMEM((2, 2, ROWS, half), BF16),
            pltpu.VMEM((4, 4, ROWS, half), BF16),
            pltpu.SemaphoreType.DMA((wide // 256 + 3,)),
            pltpu.SemaphoreType.DMA,
            pltpu.SemaphoreType.DMA((2, 2)),
            pltpu.SemaphoreType.DMA((12, 2)),
            pltpu.SemaphoreType.DMA((12, 4)),
        ],
        compiler_params=pltpu.CompilerParams(vmem_limit_bytes=VMEM, collective_id=0, has_side_effects=True),
        cost_estimate=pl.CostEstimate(
            flops=2 * rows * d * (2 * wide + 2 * kv * HEAD) + 2 * rows * rows * wide, transcendentals=rows * rows * wide // HEAD // 2,
            bytes_accessed=2 * (2 * d * wide + 2 * d * kv * HEAD + 2 * rows * d)),
        name="layer",
    )(freq, gain, x, wq, wk, wv, wo)


def solution(mesh):
    n = mesh.shape["tp"]

    def step(x, gain, wq, wk, wv, wo):
        half = HEAD // 2
        freq = THETA ** (-jnp.arange(half, dtype=F32) / half)
        freq = jnp.concatenate([freq, freq]).reshape(1, HEAD)
        return layer(x, gain.reshape(1, -1), freq, wq, wk, wv, wo, n, "tp")

    tokens, columns = P("dp", None), P(None, "tp")
    return jax.shard_map(
        step,
        mesh=mesh,
        in_specs=(tokens, P(None), columns, columns, columns, P("tp", None)),
        out_specs=tokens,
        check_vma=False,
    )
```

```python
import functools

import jax
import jax.numpy as jnp
import numpy as np
from jax import lax
from jax.experimental import pallas as pl
from jax.experimental.pallas import tpu as pltpu
from jax.sharding import PartitionSpec as P

HEAD = 128
THETA = 10000
NEG = -1e30
HIDDEN = 2 * NEG
LOG2E = 1.4426950408889634
VMEM = 67_000_000
ROWS = 128
KEYS = 256
F32, BF16 = jnp.float32, jnp.bfloat16
OB, OA, RA, LB, RB, LA, YBR, YAR, YAL, YBL, FWR, FWL = range(12)


def _dot(a, b, ca, cb):
    return lax.dot_general(a, b, (((ca,), (cb,)), ((), ())), preferred_element_type=F32)


def _kernel(freq_ref, gain_ref, x_hbm, wq_hbm, wk_hbm, wv_hbm, wo_hbm, y_hbm,
            wq, wkv, wo, gain_s, x_s, h_s, xown_s, cos_s, sin_s, q_s, k_s, vt_s, top_s, mix_s, seen_s,
            mid_s, own_s, term_s, pass_s, fin_s, got_s, far_s,
            w_sem, x_sem, y_sem, send_sem, recv_sem, *, n, axis):
    rows, d = x_hbm.shape
    chunks = rows // ROWS
    wide = wq.shape[1]
    kv = wk_hbm.shape[1] // HEAD
    g = wide // HEAD // kv
    part, half = d // n, d // n // 2
    cols = g * ROWS
    strip = cols // 2
    e = HEAD**-0.5 * LOG2E
    i = lax.axis_index(axis)
    r, l, o = lax.rem(i + 1, n), lax.rem(i + n - 1, n), lax.rem(i + 2, n)

    def column(owner, b):
        return pl.ds(pl.multiple_of(owner * part + b * half, 128), half)

    def columns(owner):
        return pl.ds(pl.multiple_of(owner * part, 128), part)

    def row(c):
        return pl.ds(pl.multiple_of(c * ROWS, ROWS), ROWS)

    def remote(kind, c):
        s2, s4 = lax.rem(c, 2), lax.rem(c, 4)
        to = r if kind in (OB, RA, RB, YBR, YAR, FWR) else l
        if kind in (OB, OA):
            src, dst = term_s.at[s2, kind], got_s.at[s2, kind]
        elif kind in (RA, LB):
            src, dst = term_s.at[s2, kind], far_s.at[s4, kind - RA]
        elif kind in (RB, LA):
            src, dst = pass_s.at[s2, kind - RB], far_s.at[s4, kind - RA]
        elif kind in (YBR, YBL):
            src, dst = fin_s.at[s2, 1], y_hbm.at[row(c), column(i, 1)]
        elif kind in (YAR, YAL):
            src, dst = fin_s.at[s2, 0], y_hbm.at[row(c), column(i, 0)]
        elif kind == FWR:
            src = dst = y_hbm.at[row(c), column(l, 1)]
        else:
            src = dst = y_hbm.at[row(c), column(r, 0)]
        return pltpu.make_async_remote_copy(
            src_ref=src, dst_ref=dst, send_sem=send_sem.at[kind, s2], recv_sem=recv_sem.at[kind, s4],
            device_id={axis: to}, device_id_type=pl.DeviceIdType.MESH,
        )

    def local(c, b):
        s2 = lax.rem(c, 2)
        return pltpu.make_async_copy(fin_s.at[s2, b], y_hbm.at[row(c), column(i, b)], y_sem.at[b, s2])

    def chunk_in(c):
        return pltpu.make_async_copy(x_hbm.at[row(c), :], x_s, x_sem)

    tile = 512
    q_tiles = [pltpu.make_async_copy(wq_hbm.at[:, pl.ds(t * tile, tile)], wq.at[:, pl.ds(t * tile, tile)], w_sem.at[t]) for t in range(wide // tile)]
    k_in = pltpu.make_async_copy(wk_hbm, wkv.at[:, : kv * HEAD], w_sem.at[len(q_tiles)])
    v_in = pltpu.make_async_copy(wv_hbm, wkv.at[:, kv * HEAD :], w_sem.at[len(q_tiles) + 1])
    owners = (o, r, l, i)
    o_tiles = [pltpu.make_async_copy(wo_hbm.at[:, columns(t)], wo.at[:, columns(t)], w_sem.at[len(q_tiles) + 2 + p]) for p, t in enumerate(owners)]

    chunk_in(0).start()
    k_in.start()
    v_in.start()
    for copy in q_tiles:
        copy.start()
    barrier = pltpu.get_barrier_semaphore()
    for to in (l, r):
        pl.semaphore_signal(barrier, inc=1, device_id={axis: to}, device_id_type=pl.DeviceIdType.MESH)

    for t in range(d // 128):
        gain_s[:, t * 128 : (t + 1) * 128] = gain_ref[t : t + 1, :].astype(F32)
    k_s[...] = jnp.zeros(k_s.shape, BF16)
    for m in range(kv):
        vt_s[m, :HEAD, :] = jnp.zeros((HEAD, rows), BF16)
        vt_s[m, HEAD:, :] = jnp.ones((vt_s.shape[1] - HEAD, rows), BF16)
    pl.semaphore_wait(barrier, 2)

    def project(c):
        chunk_in(c).wait()

        def norm(t, _):
            at = pl.ds(pl.multiple_of(t * 16, 16), 16)
            w = x_s[at, :].astype(F32)
            scale = lax.rsqrt(jnp.mean(w * w, -1, keepdims=True) + 1e-6)
            h_s[at, :] = (w * scale * gain_s[...]).astype(BF16)

        lax.fori_loop(0, ROWS // 16, norm, None)
        xown_s[...] = x_s[:, columns(i)]

        @pl.when(c + 1 < chunks)
        def _():
            chunk_in(c + 1).start()

        place = lax.broadcasted_iota(jnp.int32, (ROWS, HEAD), 0) + c * ROWS
        angle = place.astype(F32) * freq_ref[...]
        sign = jnp.where(lax.broadcasted_iota(jnp.int32, (ROWS, HEAD), 1) < HEAD // 2, -1.0, 1.0)
        cos_s[...] = jnp.cos(angle)
        sin_s[...] = jnp.sin(angle) * sign

        def first(copy):
            @pl.when(c == 0)
            def _():
                copy.wait()

        def turned(t):
            t = t.astype(BF16).astype(F32)
            return (t * cos_s[...] + pltpu.roll(t, HEAD // 2, 1) * sin_s[...]).astype(BF16)

        first(k_in)
        first(v_in)
        t = _dot(h_s[...], wkv[...], 1, 0)
        for m in range(kv):
            k_s[row(c), m * HEAD : (m + 1) * HEAD] = turned(t[:, m * HEAD : (m + 1) * HEAD])
            vt_s[m, :HEAD, row(c)] = t[:, (kv + m) * HEAD : (kv + m + 1) * HEAD].T.astype(BF16)
        for p, copy in enumerate(q_tiles):
            first(copy)
            if p == 0:
                for later in o_tiles:

                    @pl.when(c == 0)
                    def _(later=later):
                        later.start()

            t = _dot(h_s[...], wq[:, p * tile : (p + 1) * tile], 1, 0)
            for m in range(tile // HEAD):
                head = p * (tile // HEAD) + m
                q_s[head // g, head % g * ROWS : (head % g + 1) * ROWS, :] = turned(t[:, m * HEAD : (m + 1) * HEAD])

    def attend(c):
        pieces = [(m, at) for m in range(kv) for at in range(0, cols, strip)]
        top_s[...] = jnp.full(top_s.shape, NEG, F32)
        mix_s[...] = jnp.zeros(mix_s.shape, F32)

        def block(j, masked):
            here = pl.ds(pl.multiple_of(j * KEYS, KEYS), KEYS)
            scores = [_dot(k_s[here, m * HEAD : (m + 1) * HEAD], q_s[m, at : at + strip, :], 1, 1) for m, at in pieces]
            if masked:
                query = lax.rem(lax.broadcasted_iota(jnp.int32, (KEYS, strip), 1), ROWS) + c * ROWS
                ok = query >= lax.broadcasted_iota(jnp.int32, (KEYS, strip), 0) + j * KEYS
            weights, keeps = [], []
            for (m, at), s in zip(pieces, scores):
                if masked:
                    s = jnp.where(ok, s, HIDDEN)
                old = top_s[m : m + 1, at : at + strip]
                top = jnp.maximum(old, s.max(axis=0, keepdims=True))
                top_s[m : m + 1, at : at + strip] = top
                weights.append(jnp.exp2((s - top) * e).astype(BF16))
                keeps.append(jnp.exp2((old - top) * e))
            for (m, at), p, keep in zip(pieces, weights, keeps):
                mix_s[m, :, at : at + strip] = mix_s[m, :, at : at + strip] * keep + _dot(vt_s[m, :, here], p, 1, 0)

        whole = lax.div(c * ROWS, KEYS)
        lax.fori_loop(0, whole, lambda j, _: block(j, False), None)
        block(whole, True)
        for m in range(kv):
            out = (mix_s[m, :HEAD, :] * (1 / mix_s[m, HEAD : HEAD + 1, :])).T.astype(BF16)
            for h in range(g):
                at = (m * g + h) * HEAD
                seen_s[:, at : at + HEAD] = out[h * ROWS : (h + 1) * ROWS, :]

    def terms(c):
        s2 = lax.rem(c, 2)

        def product(p):
            @pl.when(c == 0)
            def _():
                o_tiles[p].wait()

            return _dot(seen_s[...], wo[:, columns(owners[p])], 1, 0)

        @pl.when(c >= 2)
        def _():
            for kind in (OB, OA, RA, LB):
                remote(kind, c - 2).wait_send()

        t = product(0)
        term_s[s2, OB], term_s[s2, OA] = t[:, half:].astype(BF16), t[:, :half].astype(BF16)
        remote(OB, c).start()
        remote(OA, c).start()
        t = product(1)
        term_s[s2, RA], mid_s[0] = t[:, :half].astype(BF16), t[:, half:]
        remote(RA, c).start()
        t = product(2)
        term_s[s2, LB], mid_s[1] = t[:, half:].astype(BF16), t[:, :half]
        remote(LB, c).start()
        t = product(3)
        for b in range(2):
            own_s[s2, b] = xown_s[:, b * half : (b + 1) * half].astype(F32) + t[:, b * half : (b + 1) * half]

    def pass_on(c):
        s2 = lax.rem(c, 2)

        @pl.when(c >= 2)
        def _():
            for kind in (RB, LA):
                remote(kind, c - 2).wait_send()

        for kind in (OB, OA):
            remote(kind, c).wait_recv()
            pass_s[s2, kind] = (mid_s[kind] + got_s[s2, kind].astype(F32)).astype(BF16)
        for kind in (RB, LA):
            remote(kind, c).start()

    def finish(c):
        s2, s4 = lax.rem(c, 2), lax.rem(c, 4)

        @pl.when(c >= 2)
        def _():
            for kind in (YBR, YAR, YAL, YBL):
                remote(kind, c - 2).wait_send()
            for b in range(2):
                local(c - 2, b).wait()

        for kind in (RA, LB, RB, LA):
            remote(kind, c).wait_recv()
        fin_s[s2, 1] = (own_s[s2, 1] + far_s[s4, LB - RA].astype(F32) + far_s[s4, RB - RA].astype(F32)).astype(BF16)
        fin_s[s2, 0] = (own_s[s2, 0] + far_s[s4, RA - RA].astype(F32) + far_s[s4, LA - RA].astype(F32)).astype(BF16)
        for kind in (YBR, YAL, YAR, YBL):
            remote(kind, c).start()
        for b in range(2):
            local(c, b).start()

    def forward(c):
        @pl.when(c >= 2)
        def _():
            for kind in (FWR, FWL):
                remote(kind, c - 2).wait_send()

        for kind, after in ((FWR, YBR), (FWL, YAL)):
            remote(after, c).wait_recv()
            remote(kind, c).start()

    def arrive(c):
        for kind in (YAR, YBL, FWR, FWL):
            remote(kind, c).wait_recv()

    def turn(c, _):
        def when(lag, do):
            @pl.when((c >= lag) & (c < chunks + lag))
            def _():
                do(c - lag)

        when(0, project)
        when(2, finish)
        when(0, attend)
        when(1, pass_on)
        when(0, terms)
        when(3, forward)
        when(4, arrive)

    lax.fori_loop(0, chunks + 5, turn, None)
    for c in (chunks - 2, chunks - 1):
        for kind in range(12):
            remote(kind, c).wait_send()
        for b in range(2):
            local(c, b).wait()


def layer(x, gain, freq, wq, wk, wv, wo, n, axis):
    rows, d = x.shape
    wide, kv = wq.shape[1], wk.shape[1] // HEAD
    g = wide // HEAD // kv
    half = d // n // 2
    cols = g * ROWS
    vmem, hbm = pl.BlockSpec(memory_space=pltpu.VMEM), pl.BlockSpec(memory_space=pl.ANY)
    return pl.pallas_call(
        functools.partial(_kernel, n=n, axis=axis),
        in_specs=[vmem, vmem] + [hbm] * 5,
        out_specs=hbm,
        out_shape=jax.ShapeDtypeStruct((rows, d), BF16),
        scratch_shapes=[
            pltpu.VMEM(wq.shape, BF16),
            pltpu.VMEM((d, 2 * kv * HEAD), BF16),
            pltpu.VMEM(wo.shape, BF16),
            pltpu.VMEM((1, d), F32),
            pltpu.VMEM((ROWS, d), BF16),
            pltpu.VMEM((ROWS, d), BF16),
            pltpu.VMEM((ROWS, d // n), BF16),
            pltpu.VMEM((ROWS, HEAD), F32),
            pltpu.VMEM((ROWS, HEAD), F32),
            pltpu.VMEM((kv, cols, HEAD), BF16),
            pltpu.VMEM((rows, kv * HEAD), BF16),
            pltpu.VMEM((kv, HEAD + 16, rows), BF16),
            pltpu.VMEM((kv, cols), F32),
            pltpu.VMEM((kv, HEAD + 16, cols), F32),
            pltpu.VMEM((ROWS, wide), BF16),
            pltpu.VMEM((2, ROWS, half), F32),
            pltpu.VMEM((2, 2, ROWS, half), F32),
            pltpu.VMEM((2, 4, ROWS, half), BF16),
            pltpu.VMEM((2, 2, ROWS, half), BF16),
            pltpu.VMEM((2, 2, ROWS, half), BF16),
            pltpu.VMEM((2, 2, ROWS, half), BF16),
            pltpu.VMEM((4, 4, ROWS, half), BF16),
            pltpu.SemaphoreType.DMA((wide // 256 + 10,)),
            pltpu.SemaphoreType.DMA,
            pltpu.SemaphoreType.DMA((2, 2)),
            pltpu.SemaphoreType.DMA((12, 2)),
            pltpu.SemaphoreType.DMA((12, 4)),
        ],
        compiler_params=pltpu.CompilerParams(vmem_limit_bytes=VMEM, collective_id=0, has_side_effects=True),
        cost_estimate=pl.CostEstimate(
            flops=2 * rows * d * (2 * wide + 2 * kv * HEAD) + 2 * rows * rows * wide, transcendentals=rows * rows * wide // HEAD // 2,
            bytes_accessed=2 * (2 * d * wide + 2 * d * kv * HEAD + 2 * rows * d)),
        name="layer",
    )(freq, gain, x, wq, wk, wv, wo)


def _settle(from_ref, to_ref, room, in_sem, out_sem):
    pieces, size = room.shape[:2]
    ins = [pltpu.make_async_copy(from_ref.at[pl.ds(t * size, size), :], room.at[t], in_sem.at[t]) for t in range(pieces)]
    outs = [pltpu.make_async_copy(room.at[t], to_ref.at[pl.ds(t * size, size), :], out_sem.at[t]) for t in range(pieces)]
    for copy in ins:
        copy.start()
    for t in range(pieces):
        ins[t].wait()
        outs[t].start()
    for copy in outs:
        copy.wait()


def settle(y):
    rows, d = y.shape
    pieces = rows // ROWS
    hbm = pl.BlockSpec(memory_space=pl.ANY)
    return pl.pallas_call(
        _settle,
        in_specs=[hbm],
        out_specs=hbm,
        out_shape=jax.ShapeDtypeStruct(y.shape, y.dtype),
        scratch_shapes=[pltpu.VMEM((pieces, ROWS, d), y.dtype), pltpu.SemaphoreType.DMA((pieces,)), pltpu.SemaphoreType.DMA((pieces,))],
        compiler_params=pltpu.CompilerParams(vmem_limit_bytes=VMEM),
        cost_estimate=pl.CostEstimate(flops=rows * d, transcendentals=0, bytes_accessed=4 * rows * d),
        name="settle",
    )(y)


def solution(mesh):
    n = mesh.shape["tp"]

    def step(x, gain, wq, wk, wv, wo):
        half = HEAD // 2
        freq = np.float32(THETA) ** (-np.arange(half, dtype=np.float32) / np.float32(half))
        freq = jnp.asarray(np.concatenate([freq, freq]).reshape(1, HEAD))
        return settle(layer(x, gain.reshape(-1, 128), freq, wq, wk, wv, wo, n, "tp"))

    tokens, columns = P("dp", None), P(None, "tp")
    return jax.shard_map(
        step,
        mesh=mesh,
        in_specs=(tokens, P(None), columns, columns, columns, P("tp", None)),
        out_specs=tokens,
        check_vma=False,
    )
```

```python
import functools

import jax
import jax.numpy as jnp
import numpy as np
from jax import lax
from jax.experimental import pallas as pl
from jax.experimental.pallas import tpu as pltpu
from jax.sharding import PartitionSpec as P

HEAD = 128
THETA = 10000
NEG = -1e30
HIDDEN = 2 * NEG
LOG2E = 1.4426950408889634
VMEM = 67_000_000
ROWS = 128
KEYS = 256
LAST = 3
F32, BF16 = jnp.float32, jnp.bfloat16
OB, OA, RA, LB, RB, LA, YBR, YAR, YAL, YBL, FWR, FWL = range(12)


def _dot(a, b, ca, cb):
    return lax.dot_general(a, b, (((ca,), (cb,)), ((), ())), preferred_element_type=F32)


def _kernel(freq_ref, gain_ref, x_hbm, wq_hbm, wk_hbm, wv_hbm, wo_hbm, y_hbm, fa_hbm, fb_hbm,
            wq, wkv, wo, gain_s, x_s, h_s, xown_s, cos_s, sin_s, q_s, k_s, vt_s, top_s, mix_s, seen_s,
            mid_s, own_s, term_s, pass_s, fin_s, got_s, far_s,
            w_sem, x_sem, y_sem, send_sem, recv_sem, *, n, axis):
    rows, d = x_hbm.shape
    chunks = rows // ROWS
    spread = chunks - LAST
    wide = wq.shape[1]
    kv = wk_hbm.shape[1] // HEAD
    g = wide // HEAD // kv
    part, half = d // n, d // n // 2
    cols = g * ROWS
    strip = cols // 2
    e = HEAD**-0.5 * LOG2E
    i = lax.axis_index(axis)
    r, l, o = lax.rem(i + 1, n), lax.rem(i + n - 1, n), lax.rem(i + 2, n)

    def column(owner, b):
        return pl.ds(pl.multiple_of(owner * part + b * half, 128), half)

    def columns(owner):
        return pl.ds(pl.multiple_of(owner * part, 128), part)

    def row(c):
        return pl.ds(pl.multiple_of(c * ROWS, ROWS), ROWS)

    def remote(kind, c):
        s2, s4 = lax.rem(c, 2), lax.rem(c, 4)
        to = r if kind in (OB, RA, RB, YBR, YAR, FWR) else l
        if kind in (OB, OA):
            src, dst = term_s.at[s2, kind], got_s.at[s2, kind]
        elif kind in (RA, LB):
            src, dst = term_s.at[s2, kind], far_s.at[s4, kind - RA]
        elif kind in (RB, LA):
            src, dst = pass_s.at[s2, kind - RB], far_s.at[s4, kind - RA]
        elif kind in (YBR, YBL):
            src, dst = fin_s.at[s2, 1], y_hbm.at[row(c), column(i, 1)]
        elif kind in (YAR, YAL):
            src, dst = fin_s.at[s2, 0], y_hbm.at[row(c), column(i, 0)]
        elif kind == FWR:
            src = dst = y_hbm.at[row(c), column(l, 1)]
        else:
            src = dst = y_hbm.at[row(c), column(r, 0)]
        return pltpu.make_async_remote_copy(
            src_ref=src, dst_ref=dst, send_sem=send_sem.at[kind, s2], recv_sem=recv_sem.at[kind, s4],
            device_id={axis: to}, device_id_type=pl.DeviceIdType.MESH,
        )

    def local(c, b, here=True):
        to = y_hbm.at[row(c), column(i, b)] if here else (fa_hbm, fb_hbm)[b].at[row(c - spread), :]
        s2 = lax.rem(c, 2)
        return pltpu.make_async_copy(fin_s.at[s2, b], to, y_sem.at[b, s2])

    def chunk_in(c):
        return pltpu.make_async_copy(x_hbm.at[row(c), :], x_s, x_sem)

    tile = 512
    q_tiles = [pltpu.make_async_copy(wq_hbm.at[:, pl.ds(t * tile, tile)], wq.at[:, pl.ds(t * tile, tile)], w_sem.at[t]) for t in range(wide // tile)]
    k_in = pltpu.make_async_copy(wk_hbm, wkv.at[:, : kv * HEAD], w_sem.at[len(q_tiles)])
    v_in = pltpu.make_async_copy(wv_hbm, wkv.at[:, kv * HEAD :], w_sem.at[len(q_tiles) + 1])
    owners = (o, r, l, i)
    o_tiles = [pltpu.make_async_copy(wo_hbm.at[:, columns(t)], wo.at[:, columns(t)], w_sem.at[len(q_tiles) + 2 + p]) for p, t in enumerate(owners)]

    chunk_in(0).start()
    k_in.start()
    v_in.start()
    for copy in q_tiles:
        copy.start()
    barrier = pltpu.get_barrier_semaphore()
    for to in (l, r):
        pl.semaphore_signal(barrier, inc=1, device_id={axis: to}, device_id_type=pl.DeviceIdType.MESH)

    for t in range(d // 128):
        gain_s[:, t * 128 : (t + 1) * 128] = gain_ref[t : t + 1, :].astype(F32)
    k_s[...] = jnp.zeros(k_s.shape, BF16)
    for m in range(kv):
        vt_s[m, :HEAD, :] = jnp.zeros((HEAD, rows), BF16)
        vt_s[m, HEAD:, :] = jnp.ones((vt_s.shape[1] - HEAD, rows), BF16)
    pl.semaphore_wait(barrier, 2)

    def project(c):
        chunk_in(c).wait()

        def norm(t, _):
            at = pl.ds(pl.multiple_of(t * 16, 16), 16)
            w = x_s[at, :].astype(F32)
            scale = lax.rsqrt(jnp.mean(w * w, -1, keepdims=True) + 1e-6)
            h_s[at, :] = (w * scale * gain_s[...]).astype(BF16)

        lax.fori_loop(0, ROWS // 16, norm, None)
        xown_s[...] = x_s[:, columns(i)]

        @pl.when(c + 1 < chunks)
        def _():
            chunk_in(c + 1).start()

        place = lax.broadcasted_iota(jnp.int32, (ROWS, HEAD), 0) + c * ROWS
        angle = place.astype(F32) * freq_ref[...]
        sign = jnp.where(lax.broadcasted_iota(jnp.int32, (ROWS, HEAD), 1) < HEAD // 2, -1.0, 1.0)
        cos_s[...] = jnp.cos(angle)
        sin_s[...] = jnp.sin(angle) * sign

        def first(copy):
            @pl.when(c == 0)
            def _():
                copy.wait()

        def turned(t):
            t = t.astype(BF16).astype(F32)
            return (t * cos_s[...] + pltpu.roll(t, HEAD // 2, 1) * sin_s[...]).astype(BF16)

        first(k_in)
        first(v_in)
        t = _dot(h_s[...], wkv[...], 1, 0)
        for m in range(kv):
            k_s[row(c), m * HEAD : (m + 1) * HEAD] = turned(t[:, m * HEAD : (m + 1) * HEAD])
            vt_s[m, :HEAD, row(c)] = t[:, (kv + m) * HEAD : (kv + m + 1) * HEAD].T.astype(BF16)
        for p, copy in enumerate(q_tiles):
            first(copy)
            if p == 0:
                for later in o_tiles:

                    @pl.when(c == 0)
                    def _(later=later):
                        later.start()

            t = _dot(h_s[...], wq[:, p * tile : (p + 1) * tile], 1, 0)
            for m in range(tile // HEAD):
                head = p * (tile // HEAD) + m
                q_s[head // g, head % g * ROWS : (head % g + 1) * ROWS, :] = turned(t[:, m * HEAD : (m + 1) * HEAD])

    def attend(c):
        pieces = [(m, at) for m in range(kv) for at in range(0, cols, strip)]
        top_s[...] = jnp.full(top_s.shape, NEG, F32)
        mix_s[...] = jnp.zeros(mix_s.shape, F32)

        def block(j, masked):
            here = pl.ds(pl.multiple_of(j * KEYS, KEYS), KEYS)
            scores = [_dot(k_s[here, m * HEAD : (m + 1) * HEAD], q_s[m, at : at + strip, :], 1, 1) for m, at in pieces]
            if masked:
                query = lax.rem(lax.broadcasted_iota(jnp.int32, (KEYS, strip), 1), ROWS) + c * ROWS
                ok = query >= lax.broadcasted_iota(jnp.int32, (KEYS, strip), 0) + j * KEYS
            weights, keeps = [], []
            for (m, at), s in zip(pieces, scores):
                if masked:
                    s = jnp.where(ok, s, HIDDEN)
                old = top_s[m : m + 1, at : at + strip]
                top = jnp.maximum(old, s.max(axis=0, keepdims=True))
                top_s[m : m + 1, at : at + strip] = top
                weights.append(jnp.exp2((s - top) * e).astype(BF16))
                keeps.append(jnp.exp2((old - top) * e))
            for (m, at), p, keep in zip(pieces, weights, keeps):
                mix_s[m, :, at : at + strip] = mix_s[m, :, at : at + strip] * keep + _dot(vt_s[m, :, here], p, 1, 0)

        whole = lax.div(c * ROWS, KEYS)
        lax.fori_loop(0, whole, lambda j, _: block(j, False), None)
        block(whole, True)
        for m in range(kv):
            out = (mix_s[m, :HEAD, :] * (1 / mix_s[m, HEAD : HEAD + 1, :])).T.astype(BF16)
            for h in range(g):
                at = (m * g + h) * HEAD
                seen_s[:, at : at + HEAD] = out[h * ROWS : (h + 1) * ROWS, :]

    def terms(c):
        s2 = lax.rem(c, 2)

        def product(p):
            @pl.when(c == 0)
            def _():
                o_tiles[p].wait()

            return _dot(seen_s[...], wo[:, columns(owners[p])], 1, 0)

        @pl.when(c >= 2)
        def _():
            for kind in (OB, OA, RA, LB):
                remote(kind, c - 2).wait_send()

        t = product(0)
        term_s[s2, OB], term_s[s2, OA] = t[:, half:].astype(BF16), t[:, :half].astype(BF16)
        remote(OB, c).start()
        remote(OA, c).start()
        t = product(1)
        term_s[s2, RA], mid_s[0] = t[:, :half].astype(BF16), t[:, half:]
        remote(RA, c).start()
        t = product(2)
        term_s[s2, LB], mid_s[1] = t[:, half:].astype(BF16), t[:, :half]
        remote(LB, c).start()
        t = product(3)
        for b in range(2):
            own_s[s2, b] = xown_s[:, b * half : (b + 1) * half].astype(F32) + t[:, b * half : (b + 1) * half]

    def pass_on(c):
        s2 = lax.rem(c, 2)

        @pl.when(c >= 2)
        def _():
            for kind in (RB, LA):
                remote(kind, c - 2).wait_send()

        for kind in (OB, OA):
            remote(kind, c).wait_recv()
            pass_s[s2, kind] = (mid_s[kind] + got_s[s2, kind].astype(F32)).astype(BF16)
        for kind in (RB, LA):
            remote(kind, c).start()

    def finish(c):
        s2, s4 = lax.rem(c, 2), lax.rem(c, 4)

        @pl.when((c >= 2) & (c < spread + 2))
        def _():
            for kind in (YBR, YAR, YAL, YBL):
                remote(kind, c - 2).wait_send()
            for b in range(2):
                local(c - 2, b).wait()

        @pl.when(c >= spread + 2)
        def _():
            for b in range(2):
                local(c - 2, b, False).wait()

        for kind in (RA, LB, RB, LA):
            remote(kind, c).wait_recv()
        fin_s[s2, 1] = (own_s[s2, 1] + far_s[s4, LB - RA].astype(F32) + far_s[s4, RB - RA].astype(F32)).astype(BF16)
        fin_s[s2, 0] = (own_s[s2, 0] + far_s[s4, RA - RA].astype(F32) + far_s[s4, LA - RA].astype(F32)).astype(BF16)
        @pl.when(c < spread)
        def _():
            for kind in (YBR, YAL, YAR, YBL):
                remote(kind, c).start()
            for b in range(2):
                local(c, b).start()

        @pl.when(c >= spread)
        def _():
            for b in range(2):
                local(c, b, False).start()

    def forward(c):
        @pl.when(c >= 2)
        def _():
            for kind in (FWR, FWL):
                remote(kind, c - 2).wait_send()

        for kind, after in ((FWR, YBR), (FWL, YAL)):
            remote(after, c).wait_recv()
            remote(kind, c).start()

    def arrive(c):
        for kind in (YAR, YBL, FWR, FWL):
            remote(kind, c).wait_recv()

    def turn(c, _):
        def when(lag, do, end=chunks):
            @pl.when((c >= lag) & (c < end + lag))
            def _():
                do(c - lag)

        when(0, project)
        when(2, finish)
        when(0, attend)
        when(1, pass_on)
        when(0, terms)
        when(3, forward, spread)
        when(4, arrive, spread)

    lax.fori_loop(0, chunks + 2, turn, None)
    for c in (chunks - 2, chunks - 1):
        for kind in (OB, OA, RA, LB, RB, LA):
            remote(kind, c).wait_send()
        for b in range(2):
            local(c, b, False).wait()
    for c in (spread - 2, spread - 1):
        for kind in (FWR, FWL):
            remote(kind, c).wait_send()


def layer(x, gain, freq, wq, wk, wv, wo, n, axis):
    rows, d = x.shape
    wide, kv = wq.shape[1], wk.shape[1] // HEAD
    g = wide // HEAD // kv
    half = d // n // 2
    cols = g * ROWS
    vmem, hbm = pl.BlockSpec(memory_space=pltpu.VMEM), pl.BlockSpec(memory_space=pl.ANY)
    return pl.pallas_call(
        functools.partial(_kernel, n=n, axis=axis),
        in_specs=[vmem, vmem] + [hbm] * 5,
        out_specs=[hbm] * 3,
        out_shape=[jax.ShapeDtypeStruct((rows, d), BF16)] + [jax.ShapeDtypeStruct((LAST * ROWS, half), BF16)] * 2,
        scratch_shapes=[
            pltpu.VMEM(wq.shape, BF16),
            pltpu.VMEM((d, 2 * kv * HEAD), BF16),
            pltpu.VMEM(wo.shape, BF16),
            pltpu.VMEM((1, d), F32),
            pltpu.VMEM((ROWS, d), BF16),
            pltpu.VMEM((ROWS, d), BF16),
            pltpu.VMEM((ROWS, d // n), BF16),
            pltpu.VMEM((ROWS, HEAD), F32),
            pltpu.VMEM((ROWS, HEAD), F32),
            pltpu.VMEM((kv, cols, HEAD), BF16),
            pltpu.VMEM((rows, kv * HEAD), BF16),
            pltpu.VMEM((kv, HEAD + 16, rows), BF16),
            pltpu.VMEM((kv, cols), F32),
            pltpu.VMEM((kv, HEAD + 16, cols), F32),
            pltpu.VMEM((ROWS, wide), BF16),
            pltpu.VMEM((2, ROWS, half), F32),
            pltpu.VMEM((2, 2, ROWS, half), F32),
            pltpu.VMEM((2, 4, ROWS, half), BF16),
            pltpu.VMEM((2, 2, ROWS, half), BF16),
            pltpu.VMEM((2, 2, ROWS, half), BF16),
            pltpu.VMEM((2, 2, ROWS, half), BF16),
            pltpu.VMEM((4, 4, ROWS, half), BF16),
            pltpu.SemaphoreType.DMA((wide // 256 + 10,)),
            pltpu.SemaphoreType.DMA,
            pltpu.SemaphoreType.DMA((2, 2)),
            pltpu.SemaphoreType.DMA((12, 2)),
            pltpu.SemaphoreType.DMA((12, 4)),
        ],
        compiler_params=pltpu.CompilerParams(vmem_limit_bytes=VMEM, collective_id=0, has_side_effects=True),
        cost_estimate=pl.CostEstimate(
            flops=2 * rows * d * (2 * wide + 2 * kv * HEAD) + 2 * rows * rows * wide, transcendentals=rows * rows * wide // HEAD // 2,
            bytes_accessed=2 * (2 * d * wide + 2 * d * kv * HEAD + 2 * rows * d)),
        name="layer",
    )(freq, gain, x, wq, wk, wv, wo)


def _move(pairs, sem):
    copies = [pltpu.make_async_copy(a, b, sem.at[t]) for t, (a, b) in enumerate(pairs)]
    for copy in copies:
        copy.start()
    for copy in copies:
        copy.wait()


def _settle(from_ref, to_ref, sem, *, end):
    size = end // sem.shape[0]
    _move([(from_ref.at[pl.ds(t * size, size), :], to_ref.at[pl.ds(t * size, size), :]) for t in range(sem.shape[0])], sem)


def _place(*refs, n, axis):
    blocks, (to_ref, sem) = refs[:8], refs[-2:]
    rows, half = blocks[0].shape
    i = lax.axis_index(axis)
    owners = (i, lax.rem(i + 1, n), lax.rem(i + n - 1, n), lax.rem(i + 2, n))
    at = [pl.ds(pl.multiple_of((2 * owner + b) * half, 128), half) for owner in owners for b in range(2)]
    row = pl.ds(to_ref.shape[0] - rows, rows)
    _move([(block, to_ref.at[row, t]) for block, t in zip(blocks, at)], sem)


def into(kernel, shape, given, y, copies, name):
    hbm = pl.BlockSpec(memory_space=pl.ANY)
    size = sum(t.size for t in given)
    return pl.pallas_call(
        kernel,
        in_specs=[hbm] * (len(given) + (y is not None)),
        out_specs=hbm,
        out_shape=jax.ShapeDtypeStruct(shape, BF16),
        input_output_aliases={} if y is None else {len(given): 0},
        scratch_shapes=[pltpu.SemaphoreType.DMA((copies,))],
        compiler_params=pltpu.CompilerParams(vmem_limit_bytes=2**20),
        cost_estimate=pl.CostEstimate(flops=400 * size, transcendentals=0, bytes_accessed=4 * size),
        name=name,
    )(*given, *([] if y is None else [y]))


def solution(mesh):
    n = mesh.shape["tp"]
    right = lambda t: lax.ppermute(t, "tp", [(i, (i + 1) % n) for i in range(n)])
    left = lambda t: lax.ppermute(t, "tp", [(i, (i - 1) % n) for i in range(n)])

    def step(x, gain, wq, wk, wv, wo):
        half = HEAD // 2
        freq = np.float32(THETA) ** (-np.arange(half, dtype=np.float32) / np.float32(half))
        freq = jnp.asarray(np.concatenate([freq, freq]).reshape(1, HEAD))
        rows, d = x.shape
        t, fa, fb = layer(x, gain.reshape(-1, 128), freq, wq, wk, wv, wo, n, "tp")
        l_b, r_a = right(fb), left(fa)
        l_a, r_b = right(fa), left(fb)
        y = into(functools.partial(_settle, end=rows - LAST * ROWS), x.shape, [t], None, rows // ROWS - LAST, "settle")
        l_b, r_a, y = lax.optimization_barrier((l_b, r_a, y))
        o_b, o_a = right(l_b), left(r_a)
        blocks = [fa, fb, r_a, r_b, l_a, l_b, o_a, o_b]
        return into(functools.partial(_place, n=n, axis="tp"), x.shape, blocks, y, 8, "place")

    tokens, columns = P("dp", None), P(None, "tp")
    return jax.shard_map(
        step,
        mesh=mesh,
        in_specs=(tokens, P(None), columns, columns, columns, P("tp", None)),
        out_specs=tokens,
        check_vma=False,
    )
```

```python
import functools

import jax
import jax.numpy as jnp
import numpy as np
from jax import lax
from jax.experimental import pallas as pl
from jax.experimental.pallas import tpu as pltpu
from jax.sharding import PartitionSpec as P

HEAD = 128
THETA = 10000
NEG = -1e30
HIDDEN = 2 * NEG
LOG2E = 1.4426950408889634
VMEM = 67_000_000
ROWS = 128
KEYS = 256
AHEAD = 3
LAST = 3
F32, BF16 = jnp.float32, jnp.bfloat16
OB, OA, RA, LB, RB, LA, YBR, YAR, YAL, YBL, FWR, FWL = range(12)


def _dot(a, b, ca, cb):
    return lax.dot_general(a, b, (((ca,), (cb,)), ((), ())), preferred_element_type=F32)


def _kernel(freq_ref, gain_ref, x_hbm, wq_hbm, wk_hbm, wv_hbm, wo_hbm, y_hbm, fa_hbm, fb_hbm,
            wq, wkv, wo, gain_s, x_s, h_s, xown_s, cos_s, sin_s, q_s, k_s, vt_s, top_s, mix_s, seen_s,
            mid_s, own_s, term_s, pass_s, fin_s, got_s, far_s,
            w_sem, x_sem, y_sem, send_sem, recv_sem, *, n, axis):
    rows, d = x_hbm.shape
    chunks = rows // ROWS
    spread = chunks - LAST
    wide = wq.shape[1]
    kv = wk_hbm.shape[1] // HEAD
    g = wide // HEAD // kv
    part, half = d // n, d // n // 2
    cols = g * ROWS
    strip = cols // 2
    e = HEAD**-0.5 * LOG2E
    i = lax.axis_index(axis)
    r, l, o = lax.rem(i + 1, n), lax.rem(i + n - 1, n), lax.rem(i + 2, n)

    def column(owner, b):
        return pl.ds(pl.multiple_of(owner * part + b * half, 128), half)

    def columns(owner):
        return pl.ds(pl.multiple_of(owner * part, 128), part)

    def row(c):
        return pl.ds(pl.multiple_of(c * ROWS, ROWS), ROWS)

    def remote(kind, c):
        s2, s4 = lax.rem(c, 2), lax.rem(c, 4)
        to = r if kind in (OB, RA, RB, YBR, YAR, FWR) else l
        if kind in (OB, OA):
            src, dst = term_s.at[s2, kind], got_s.at[s2, kind]
        elif kind in (RA, LB):
            src, dst = term_s.at[s2, kind], far_s.at[s4, kind - RA]
        elif kind in (RB, LA):
            src, dst = pass_s.at[s2, kind - RB], far_s.at[s4, kind - RA]
        elif kind in (YBR, YBL):
            src, dst = fin_s.at[s2, 1], y_hbm.at[row(c), column(i, 1)]
        elif kind in (YAR, YAL):
            src, dst = fin_s.at[s2, 0], y_hbm.at[row(c), column(i, 0)]
        elif kind == FWR:
            src = dst = y_hbm.at[row(c), column(l, 1)]
        else:
            src = dst = y_hbm.at[row(c), column(r, 0)]
        return pltpu.make_async_remote_copy(
            src_ref=src, dst_ref=dst, send_sem=send_sem.at[kind, s2], recv_sem=recv_sem.at[kind, s4],
            device_id={axis: to}, device_id_type=pl.DeviceIdType.MESH,
        )

    def local(c, b, here=True):
        to = y_hbm.at[row(c), column(i, b)] if here else (fa_hbm, fb_hbm)[b].at[row(c - spread), :]
        s2 = lax.rem(c, 2)
        return pltpu.make_async_copy(fin_s.at[s2, b], to, y_sem.at[b, s2])

    def chunk_in(c):
        return pltpu.make_async_copy(x_hbm.at[row(c), :], x_s, x_sem)

    tile = 512
    q_tiles = [pltpu.make_async_copy(wq_hbm.at[:, pl.ds(t * tile, tile)], wq.at[:, pl.ds(t * tile, tile)], w_sem.at[t]) for t in range(wide // tile)]
    k_in = pltpu.make_async_copy(wk_hbm, wkv.at[:, : kv * HEAD], w_sem.at[len(q_tiles)])
    v_in = pltpu.make_async_copy(wv_hbm, wkv.at[:, kv * HEAD :], w_sem.at[len(q_tiles) + 1])
    owners = (o, r, l, i)
    o_tiles = [pltpu.make_async_copy(wo_hbm.at[:, columns(t)], wo.at[:, columns(t)], w_sem.at[len(q_tiles) + 2 + p]) for p, t in enumerate(owners)]

    chunk_in(0).start()
    loads = [k_in, v_in, *q_tiles, *o_tiles]
    for copy in loads[:AHEAD]:
        copy.start()
    barrier = pltpu.get_barrier_semaphore()
    for to in (l, r):
        pl.semaphore_signal(barrier, inc=1, device_id={axis: to}, device_id_type=pl.DeviceIdType.MESH)

    for t in range(d // 128):
        gain_s[:, t * 128 : (t + 1) * 128] = gain_ref[t : t + 1, :].astype(F32)
    k_s[...] = jnp.zeros(k_s.shape, BF16)
    for m in range(kv):
        vt_s[m, :HEAD, :] = jnp.zeros((HEAD, rows), BF16)
        vt_s[m, HEAD:, :] = jnp.ones((vt_s.shape[1] - HEAD, rows), BF16)
    pl.semaphore_wait(barrier, 2)

    def turned(t):
        t = t.astype(BF16).astype(F32)
        return (t * cos_s[...] + pltpu.roll(t, HEAD // 2, 1) * sin_s[...]).astype(BF16)

    def first(c, number):
        @pl.when(c == 0)
        def _():
            loads[number].wait()
            if number + AHEAD < len(loads):
                loads[number + AHEAD].start()

    def project(c):
        chunk_in(c).wait()

        def norm(t, _):
            at = pl.ds(pl.multiple_of(t * 16, 16), 16)
            w = x_s[at, :].astype(F32)
            scale = lax.rsqrt(jnp.mean(w * w, -1, keepdims=True) + 1e-6)
            h_s[at, :] = (w * scale * gain_s[...]).astype(BF16)

        lax.fori_loop(0, ROWS // 16, norm, None)
        xown_s[...] = x_s[:, columns(i)]

        @pl.when(c + 1 < chunks)
        def _():
            chunk_in(c + 1).start()

        place = lax.broadcasted_iota(jnp.int32, (ROWS, HEAD), 0) + c * ROWS
        angle = place.astype(F32) * freq_ref[...]
        sign = jnp.where(lax.broadcasted_iota(jnp.int32, (ROWS, HEAD), 1) < HEAD // 2, -1.0, 1.0)
        cos_s[...] = jnp.cos(angle)
        sin_s[...] = jnp.sin(angle) * sign

        first(c, 0)
        first(c, 1)
        t = _dot(h_s[...], wkv[...], 1, 0)
        for m in range(kv):
            k_s[row(c), m * HEAD : (m + 1) * HEAD] = turned(t[:, m * HEAD : (m + 1) * HEAD])
            vt_s[m, :HEAD, row(c)] = t[:, (kv + m) * HEAD : (kv + m + 1) * HEAD].T.astype(BF16)
        queries(c, 0)

    def queries(c, p):
        first(c, 2 + p)
        t = _dot(h_s[...], wq[:, p * tile : (p + 1) * tile], 1, 0)
        for m in range(tile // HEAD):
            head = p * (tile // HEAD) + m
            q_s[head // g, head % g * ROWS : (head % g + 1) * ROWS, :] = turned(t[:, m * HEAD : (m + 1) * HEAD])

    def more_queries(c):
        for p in range(1, len(q_tiles)):
            queries(c, p)

    def attend(c):
        pieces = [(m, at) for m in range(kv) for at in range(0, cols, strip)]
        top_s[...] = jnp.full(top_s.shape, NEG, F32)
        mix_s[...] = jnp.zeros(mix_s.shape, F32)

        def block(j, masked):
            here = pl.ds(pl.multiple_of(j * KEYS, KEYS), KEYS)
            scores = [_dot(k_s[here, m * HEAD : (m + 1) * HEAD], q_s[m, at : at + strip, :], 1, 1) for m, at in pieces]
            if masked:
                query = lax.rem(lax.broadcasted_iota(jnp.int32, (KEYS, strip), 1), ROWS) + c * ROWS
                ok = query >= lax.broadcasted_iota(jnp.int32, (KEYS, strip), 0) + j * KEYS
            weights, keeps = [], []
            for (m, at), s in zip(pieces, scores):
                if masked:
                    s = jnp.where(ok, s, HIDDEN)
                old = top_s[m : m + 1, at : at + strip]
                top = jnp.maximum(old, s.max(axis=0, keepdims=True))
                top_s[m : m + 1, at : at + strip] = top
                weights.append(jnp.exp2((s - top) * e).astype(BF16))
                keeps.append(jnp.exp2((old - top) * e))
            for (m, at), p, keep in zip(pieces, weights, keeps):
                mix_s[m, :, at : at + strip] = mix_s[m, :, at : at + strip] * keep + _dot(vt_s[m, :, here], p, 1, 0)

        whole = lax.div(c * ROWS, KEYS)
        lax.fori_loop(0, whole, lambda j, _: block(j, False), None)
        block(whole, True)
        for m in range(kv):
            out = (mix_s[m, :HEAD, :] * (1 / mix_s[m, HEAD : HEAD + 1, :])).T.astype(BF16)
            for h in range(g):
                at = (m * g + h) * HEAD
                seen_s[:, at : at + HEAD] = out[h * ROWS : (h + 1) * ROWS, :]

    def terms(c):
        s2 = lax.rem(c, 2)

        def product(p):
            first(c, 2 + len(q_tiles) + p)
            return _dot(seen_s[...], wo[:, columns(owners[p])], 1, 0)

        @pl.when(c >= 2)
        def _():
            for kind in (OB, OA, RA, LB):
                remote(kind, c - 2).wait_send()

        t = product(0)
        term_s[s2, OB], term_s[s2, OA] = t[:, half:].astype(BF16), t[:, :half].astype(BF16)
        remote(OB, c).start()
        remote(OA, c).start()
        t = product(1)
        term_s[s2, RA], mid_s[0] = t[:, :half].astype(BF16), t[:, half:]
        remote(RA, c).start()
        t = product(2)
        term_s[s2, LB], mid_s[1] = t[:, half:].astype(BF16), t[:, :half]
        remote(LB, c).start()
        t = product(3)
        for b in range(2):
            own_s[s2, b] = xown_s[:, b * half : (b + 1) * half].astype(F32) + t[:, b * half : (b + 1) * half]

    def pass_on(c):
        s2 = lax.rem(c, 2)

        @pl.when(c >= 2)
        def _():
            for kind in (RB, LA):
                remote(kind, c - 2).wait_send()

        for kind in (OB, OA):
            remote(kind, c).wait_recv()
            pass_s[s2, kind] = (mid_s[kind] + got_s[s2, kind].astype(F32)).astype(BF16)
        for kind in (RB, LA):
            remote(kind, c).start()

    def finish(c):
        s2, s4 = lax.rem(c, 2), lax.rem(c, 4)

        @pl.when((c >= 2) & (c < spread + 2))
        def _():
            for kind in (YBR, YAR, YAL, YBL):
                remote(kind, c - 2).wait_send()
            for b in range(2):
                local(c - 2, b).wait()

        @pl.when(c >= spread + 2)
        def _():
            for b in range(2):
                local(c - 2, b, False).wait()

        for kind in (RA, LB, RB, LA):
            remote(kind, c).wait_recv()
        fin_s[s2, 1] = (own_s[s2, 1] + far_s[s4, LB - RA].astype(F32) + far_s[s4, RB - RA].astype(F32)).astype(BF16)
        fin_s[s2, 0] = (own_s[s2, 0] + far_s[s4, RA - RA].astype(F32) + far_s[s4, LA - RA].astype(F32)).astype(BF16)
        @pl.when(c < spread)
        def _():
            for kind in (YBR, YAL, YAR, YBL):
                remote(kind, c).start()
            for b in range(2):
                local(c, b).start()

        @pl.when(c >= spread)
        def _():
            for b in range(2):
                local(c, b, False).start()

    def forward(c):
        @pl.when(c >= 2)
        def _():
            for kind in (FWR, FWL):
                remote(kind, c - 2).wait_send()

        for kind, after in ((FWR, YBR), (FWL, YAL)):
            remote(after, c).wait_recv()
            remote(kind, c).start()
        for kind in (YAR, YBL):
            remote(kind, c).wait_recv()

    def arrive(c):
        for kind in (FWR, FWL):
            remote(kind, c).wait_recv()

    def turn(c, _):
        def when(lag, do, end=chunks):
            @pl.when((c >= lag) & (c < end + lag))
            def _():
                do(c - lag)

        when(0, project)

        @pl.when(c == 1)
        def _():
            pass_on(c - 1)

        when(0, more_queries)
        when(2, finish)
        when(0, attend)

        @pl.when((c > 1) & (c <= chunks))
        def _():
            pass_on(c - 1)

        when(0, terms)
        when(4, forward, spread)
        when(5, arrive, spread)

    lax.fori_loop(0, chunks + 2, turn, None)
    for c in (chunks - 2, chunks - 1):
        for kind in (OB, OA, RA, LB, RB, LA):
            remote(kind, c).wait_send()
        for b in range(2):
            local(c, b, False).wait()
    for c in (spread - 2, spread - 1):
        for kind in (FWR, FWL):
            remote(kind, c).wait_send()


def layer(x, gain, freq, wq, wk, wv, wo, n, axis):
    rows, d = x.shape
    wide, kv = wq.shape[1], wk.shape[1] // HEAD
    g = wide // HEAD // kv
    half = d // n // 2
    cols = g * ROWS
    vmem, hbm = pl.BlockSpec(memory_space=pltpu.VMEM), pl.BlockSpec(memory_space=pl.ANY)
    return pl.pallas_call(
        functools.partial(_kernel, n=n, axis=axis),
        in_specs=[vmem, vmem] + [hbm] * 5,
        out_specs=[hbm] * 3,
        out_shape=[jax.ShapeDtypeStruct((rows, d), BF16)] + [jax.ShapeDtypeStruct((LAST * ROWS, half), BF16)] * 2,
        scratch_shapes=[
            pltpu.VMEM(wq.shape, BF16),
            pltpu.VMEM((d, 2 * kv * HEAD), BF16),
            pltpu.VMEM(wo.shape, BF16),
            pltpu.VMEM((1, d), F32),
            pltpu.VMEM((ROWS, d), BF16),
            pltpu.VMEM((ROWS, d), BF16),
            pltpu.VMEM((ROWS, d // n), BF16),
            pltpu.VMEM((ROWS, HEAD), F32),
            pltpu.VMEM((ROWS, HEAD), F32),
            pltpu.VMEM((kv, cols, HEAD), BF16),
            pltpu.VMEM((rows, kv * HEAD), BF16),
            pltpu.VMEM((kv, HEAD + 16, rows), BF16),
            pltpu.VMEM((kv, cols), F32),
            pltpu.VMEM((kv, HEAD + 16, cols), F32),
            pltpu.VMEM((ROWS, wide), BF16),
            pltpu.VMEM((2, ROWS, half), F32),
            pltpu.VMEM((2, 2, ROWS, half), F32),
            pltpu.VMEM((2, 4, ROWS, half), BF16),
            pltpu.VMEM((2, 2, ROWS, half), BF16),
            pltpu.VMEM((2, 2, ROWS, half), BF16),
            pltpu.VMEM((2, 2, ROWS, half), BF16),
            pltpu.VMEM((4, 4, ROWS, half), BF16),
            pltpu.SemaphoreType.DMA((wide // 256 + 10,)),
            pltpu.SemaphoreType.DMA,
            pltpu.SemaphoreType.DMA((2, 2)),
            pltpu.SemaphoreType.DMA((12, 2)),
            pltpu.SemaphoreType.DMA((12, 4)),
        ],
        compiler_params=pltpu.CompilerParams(vmem_limit_bytes=VMEM, collective_id=0, has_side_effects=True),
        cost_estimate=pl.CostEstimate(
            flops=2 * rows * d * (2 * wide + 2 * kv * HEAD) + 2 * rows * rows * wide, transcendentals=rows * rows * wide // HEAD // 2,
            bytes_accessed=2 * (2 * d * wide + 2 * d * kv * HEAD + 2 * rows * d)),
        name="layer",
    )(freq, gain, x, wq, wk, wv, wo)


def _move(pairs, sem):
    copies = [pltpu.make_async_copy(a, b, sem.at[t]) for t, (a, b) in enumerate(pairs)]
    for copy in copies:
        copy.start()
    for copy in copies:
        copy.wait()


def _settle(from_ref, to_ref, sem, *, end):
    size = end // sem.shape[0]
    _move([(from_ref.at[pl.ds(t * size, size), :], to_ref.at[pl.ds(t * size, size), :]) for t in range(sem.shape[0])], sem)


def _place(*refs, n, axis, ahead):
    blocks, (to_ref, sem) = refs[: 2 * len(ahead)], refs[-2:]
    rows, half = blocks[0].shape
    owners = [lax.rem(lax.axis_index(axis) + t, n) for t in ahead]
    at = [pl.ds(pl.multiple_of((2 * owner + b) * half, 128), half) for owner in owners for b in range(2)]
    row = pl.ds(to_ref.shape[0] - rows, rows)
    _move([(block, to_ref.at[row, t]) for block, t in zip(blocks, at)], sem)


def into(kernel, shape, given, y, copies, name):
    hbm = pl.BlockSpec(memory_space=pl.ANY)
    size = sum(t.size for t in given)
    return pl.pallas_call(
        kernel,
        in_specs=[hbm] * (len(given) + (y is not None)),
        out_specs=hbm,
        out_shape=jax.ShapeDtypeStruct(shape, BF16),
        input_output_aliases={} if y is None else {len(given): 0},
        scratch_shapes=[pltpu.SemaphoreType.DMA((copies,))],
        compiler_params=pltpu.CompilerParams(vmem_limit_bytes=2**20),
        cost_estimate=pl.CostEstimate(flops=400 * size, transcendentals=0, bytes_accessed=4 * size),
        name=name,
    )(*given, *([] if y is None else [y]))


def solution(mesh):
    n = mesh.shape["tp"]
    right = lambda t: lax.ppermute(t, "tp", [(i, (i + 1) % n) for i in range(n)])
    left = lambda t: lax.ppermute(t, "tp", [(i, (i - 1) % n) for i in range(n)])

    def step(x, gain, wq, wk, wv, wo):
        half = HEAD // 2
        freq = np.float32(THETA) ** (-np.arange(half, dtype=np.float32) / np.float32(half))
        freq = jnp.asarray(np.concatenate([freq, freq]).reshape(1, HEAD))
        rows, d = x.shape
        t, fa, fb = layer(x, gain.reshape(-1, 128), freq, wq, wk, wv, wo, n, "tp")
        l_b, r_a = right(fb), left(fa)
        l_a, r_b = right(fa), left(fb)
        y = into(functools.partial(_settle, end=rows - LAST * ROWS), x.shape, [t], None, rows // ROWS - LAST, "settle")
        l_b, r_a, y = lax.optimization_barrier((l_b, r_a, y))
        o_b, o_a = right(l_b), left(r_a)
        place = lambda ahead, blocks, y: into(functools.partial(_place, n=n, axis="tp", ahead=ahead), x.shape, blocks, y, len(blocks), "place")
        y = place((0, 1, n - 1), [fa, fb, r_a, r_b, l_a, l_b], y)
        return place((2,), [o_a, o_b], y)

    tokens, columns = P("dp", None), P(None, "tp")
    return jax.shard_map(
        step,
        mesh=mesh,
        in_specs=(tokens, P(None), columns, columns, columns, P("tp", None)),
        out_specs=tokens,
        check_vma=False,
    )
```

```python
import functools

import jax
import jax.numpy as jnp
import numpy as np
from jax import lax
from jax.experimental import pallas as pl
from jax.experimental.pallas import tpu as pltpu
from jax.sharding import PartitionSpec as P

HEAD = 128
THETA = 10000
NEG = float(np.finfo(np.float32).min)
LOG2E = 1.4426950408889634
VMEM = 67_000_000
ROWS = 128
KEYS = 256
AHEAD = 3
LAST = 3
F32, BF16 = jnp.float32, jnp.bfloat16
OB, OA, RA, LB, RB, LA, YBR, YAR, YAL, YBL, FWR, FWL = range(12)


def _dot(a, b, ca, cb):
    return lax.dot_general(a, b, (((ca,), (cb,)), ((), ())), preferred_element_type=F32)


def _kernel(freq_ref, gain_ref, x_hbm, wq_hbm, wk_hbm, wv_hbm, wo_hbm, y_hbm, fa_hbm, fb_hbm,
            wq, wkv, wo, gain_s, x_s, h_s, xown_s, cos_s, sin_s, q_s, k_s, vt_s, top_s, mix_s, seen_s,
            mid_s, own_s, term_s, pass_s, fin_s, got_s, far_s,
            w_sem, x_sem, y_sem, send_sem, recv_sem, *, n, axis):
    rows, d = x_hbm.shape
    chunks = rows // ROWS
    spread = chunks - LAST
    wide = wq.shape[1]
    kv = wk_hbm.shape[1] // HEAD
    g = wide // HEAD // kv
    part, half = d // n, d // n // 2
    cols = g * ROWS
    strip = cols // 2
    e = HEAD**-0.5 * LOG2E
    i = lax.axis_index(axis)
    r, l, o = lax.rem(i + 1, n), lax.rem(i + n - 1, n), lax.rem(i + 2, n)

    def column(owner, b):
        return pl.ds(pl.multiple_of(owner * part + b * half, 128), half)

    def columns(owner):
        return pl.ds(pl.multiple_of(owner * part, 128), part)

    def row(c):
        return pl.ds(pl.multiple_of(c * ROWS, ROWS), ROWS)

    def remote(kind, c):
        s2, s4 = lax.rem(c, 2), lax.rem(c, 4)
        to = r if kind in (OB, RA, RB, YBR, YAR, FWR) else l
        if kind in (OB, OA):
            src, dst = term_s.at[s2, kind], got_s.at[s2, kind]
        elif kind in (RA, LB):
            src, dst = term_s.at[s2, kind], far_s.at[s4, kind - RA]
        elif kind in (RB, LA):
            src, dst = pass_s.at[s2, kind - RB], far_s.at[s4, kind - RA]
        elif kind in (YBR, YBL):
            src, dst = fin_s.at[s2, 1], y_hbm.at[row(c), column(i, 1)]
        elif kind in (YAR, YAL):
            src, dst = fin_s.at[s2, 0], y_hbm.at[row(c), column(i, 0)]
        elif kind == FWR:
            src = dst = y_hbm.at[row(c), column(l, 1)]
        else:
            src = dst = y_hbm.at[row(c), column(r, 0)]
        return pltpu.make_async_remote_copy(
            src_ref=src, dst_ref=dst, send_sem=send_sem.at[kind, s2], recv_sem=recv_sem.at[kind, s4],
            device_id={axis: to}, device_id_type=pl.DeviceIdType.MESH,
        )

    def local(c, b, here=True):
        to = y_hbm.at[row(c), column(i, b)] if here else (fa_hbm, fb_hbm)[b].at[row(c - spread), :]
        s2 = lax.rem(c, 2)
        return pltpu.make_async_copy(fin_s.at[s2, b], to, y_sem.at[b, s2])

    def chunk_in(c):
        return pltpu.make_async_copy(x_hbm.at[row(c), :], x_s, x_sem)

    tile = 512
    q_tiles = [pltpu.make_async_copy(wq_hbm.at[:, pl.ds(t * tile, tile)], wq.at[:, pl.ds(t * tile, tile)], w_sem.at[t]) for t in range(wide // tile)]
    k_in = pltpu.make_async_copy(wk_hbm, wkv.at[:, : kv * HEAD], w_sem.at[len(q_tiles)])
    v_in = pltpu.make_async_copy(wv_hbm, wkv.at[:, kv * HEAD :], w_sem.at[len(q_tiles) + 1])
    owners = (o, r, l, i)
    o_tiles = [pltpu.make_async_copy(wo_hbm.at[:, columns(t)], wo.at[:, columns(t)], w_sem.at[len(q_tiles) + 2 + p]) for p, t in enumerate(owners)]

    chunk_in(0).start()
    loads = [k_in, v_in, *q_tiles, *o_tiles]
    for copy in loads[:AHEAD]:
        copy.start()
    barrier = pltpu.get_barrier_semaphore()
    for to in (l, r):
        pl.semaphore_signal(barrier, inc=1, device_id={axis: to}, device_id_type=pl.DeviceIdType.MESH)

    for t in range(d // 128):
        gain_s[:, t * 128 : (t + 1) * 128] = gain_ref[t : t + 1, :].astype(F32)
    k_s[...] = jnp.zeros(k_s.shape, BF16)
    for m in range(kv):
        vt_s[m, :HEAD, :] = jnp.zeros((HEAD, rows), BF16)
        vt_s[m, HEAD:, :] = jnp.ones((vt_s.shape[1] - HEAD, rows), BF16)
    pl.semaphore_wait(barrier, 2)

    def turned(t):
        t = t.astype(BF16).astype(F32)
        return (t * cos_s[...] + pltpu.roll(t, HEAD // 2, 1) * sin_s[...]).astype(BF16)

    def first(c, number):
        @pl.when(c == 0)
        def _():
            loads[number].wait()
            if number + AHEAD < len(loads):
                loads[number + AHEAD].start()

    def project(c):
        chunk_in(c).wait()

        def norm(t, _):
            at = pl.ds(pl.multiple_of(t * 16, 16), 16)
            w = x_s[at, :].astype(F32)
            scale = lax.rsqrt(jnp.mean(w * w, -1, keepdims=True) + 1e-6)
            h_s[at, :] = (w * scale * gain_s[...]).astype(BF16)

        lax.fori_loop(0, ROWS // 16, norm, None)
        xown_s[...] = x_s[:, columns(i)]

        @pl.when((c > 0) & (c + 1 < chunks))
        def _():
            chunk_in(c + 1).start()

        place = lax.broadcasted_iota(jnp.int32, (ROWS, HEAD), 0) + c * ROWS
        angle = place.astype(F32) * freq_ref[...]
        sign = jnp.where(lax.broadcasted_iota(jnp.int32, (ROWS, HEAD), 1) < HEAD // 2, -1.0, 1.0)
        cos_s[...] = jnp.cos(angle)
        sin_s[...] = jnp.sin(angle) * sign

        first(c, 0)
        first(c, 1)
        t = _dot(h_s[...], wkv[...], 1, 0)
        for m in range(kv):
            k_s[row(c), m * HEAD : (m + 1) * HEAD] = turned(t[:, m * HEAD : (m + 1) * HEAD])
            vt_s[m, :HEAD, row(c)] = t[:, (kv + m) * HEAD : (kv + m + 1) * HEAD].T.astype(BF16)
        queries(c, 0)

    def queries(c, p):
        first(c, 2 + p)
        t = _dot(h_s[...], wq[:, p * tile : (p + 1) * tile], 1, 0)
        for m in range(tile // HEAD):
            head = p * (tile // HEAD) + m
            q_s[head // g, head % g * ROWS : (head % g + 1) * ROWS, :] = turned(t[:, m * HEAD : (m + 1) * HEAD])

    def more_queries(c):
        for p in range(1, len(q_tiles)):
            queries(c, p)

    def attend(c):
        pieces = [(m, at) for m in range(kv) for at in range(0, cols, strip)]
        top_s[...] = jnp.full(top_s.shape, NEG, F32)
        mix_s[...] = jnp.zeros(mix_s.shape, F32)

        def block(j, masked):
            here = pl.ds(pl.multiple_of(j * KEYS, KEYS), KEYS)
            scores = [_dot(k_s[here, m * HEAD : (m + 1) * HEAD], q_s[m, at : at + strip, :], 1, 1) for m, at in pieces]
            if masked:
                query = lax.rem(lax.broadcasted_iota(jnp.int32, (KEYS, strip), 1), ROWS) + c * ROWS
                ok = query >= lax.broadcasted_iota(jnp.int32, (KEYS, strip), 0) + j * KEYS
            weights, keeps = [], []
            for (m, at), s in zip(pieces, scores):
                if masked:
                    s = jnp.where(ok, s, NEG)
                old = top_s[m : m + 1, at : at + strip]
                top = jnp.maximum(old, s.max(axis=0, keepdims=True))
                top_s[m : m + 1, at : at + strip] = top
                weights.append(jnp.exp2((s - top) * e).astype(BF16))
                keeps.append(jnp.exp2((old - top) * e))
            for (m, at), p, keep in zip(pieces, weights, keeps):
                mix_s[m, :, at : at + strip] = mix_s[m, :, at : at + strip] * keep + _dot(vt_s[m, :, here], p, 1, 0)

        whole = lax.div(c * ROWS, KEYS)
        lax.fori_loop(0, whole, lambda j, _: block(j, False), None)
        block(whole, True)
        for m in range(kv):
            out = (mix_s[m, :HEAD, :] * (1 / mix_s[m, HEAD : HEAD + 1, :])).T.astype(BF16)
            for h in range(g):
                at = (m * g + h) * HEAD
                seen_s[:, at : at + HEAD] = out[h * ROWS : (h + 1) * ROWS, :]

    def terms(c):
        s2 = lax.rem(c, 2)

        def product(p):
            first(c, 2 + len(q_tiles) + p)
            return _dot(seen_s[...], wo[:, columns(owners[p])], 1, 0)

        @pl.when(c >= 2)
        def _():
            for kind in (OB, OA, RA, LB):
                remote(kind, c - 2).wait_send()

        t = product(0)
        term_s[s2, OB], term_s[s2, OA] = t[:, half:].astype(BF16), t[:, :half].astype(BF16)
        remote(OB, c).start()
        remote(OA, c).start()

        @pl.when(c == 0)
        def _():
            chunk_in(1).start()

        t = product(1)
        term_s[s2, RA], mid_s[0] = t[:, :half].astype(BF16), t[:, half:]
        remote(RA, c).start()
        t = product(2)
        term_s[s2, LB], mid_s[1] = t[:, half:].astype(BF16), t[:, :half]
        remote(LB, c).start()
        t = product(3)
        for b in range(2):
            own_s[s2, b] = xown_s[:, b * half : (b + 1) * half].astype(F32) + t[:, b * half : (b + 1) * half]

    def pass_on(c):
        s2 = lax.rem(c, 2)

        @pl.when(c >= 2)
        def _():
            for kind in (RB, LA):
                remote(kind, c - 2).wait_send()

        for kind in (OB, OA):
            remote(kind, c).wait_recv()
            pass_s[s2, kind] = (mid_s[kind] + got_s[s2, kind].astype(F32)).astype(BF16)
        for kind in (RB, LA):
            remote(kind, c).start()

    def finish(c):
        s2, s4 = lax.rem(c, 2), lax.rem(c, 4)

        @pl.when((c >= 2) & (c < spread + 2))
        def _():
            for kind in (YBR, YAR, YAL, YBL):
                remote(kind, c - 2).wait_send()
            for b in range(2):
                local(c - 2, b).wait()

        @pl.when(c >= spread + 2)
        def _():
            for b in range(2):
                local(c - 2, b, False).wait()

        for kind in (RA, LB, RB, LA):
            remote(kind, c).wait_recv()
        fin_s[s2, 1] = (own_s[s2, 1] + far_s[s4, LB - RA].astype(F32) + far_s[s4, RB - RA].astype(F32)).astype(BF16)
        fin_s[s2, 0] = (own_s[s2, 0] + far_s[s4, RA - RA].astype(F32) + far_s[s4, LA - RA].astype(F32)).astype(BF16)
        @pl.when(c < spread)
        def _():
            for kind in (YBR, YAL, YAR, YBL):
                remote(kind, c).start()
            for b in range(2):
                local(c, b).start()

        @pl.when(c >= spread)
        def _():
            for b in range(2):
                local(c, b, False).start()

    def forward(c):
        @pl.when(c >= 2)
        def _():
            for kind in (FWR, FWL):
                remote(kind, c - 2).wait_send()

        for kind, after in ((FWR, YBR), (FWL, YAL)):
            remote(after, c).wait_recv()
            remote(kind, c).start()
        for kind in (YAR, YBL):
            remote(kind, c).wait_recv()

    def arrive(c):
        for kind in (FWR, FWL):
            remote(kind, c).wait_recv()

    def turn(c, _):
        def when(lag, do, end=chunks):
            @pl.when((c >= lag) & (c < end + lag))
            def _():
                do(c - lag)

        when(0, project)

        @pl.when(c == 1)
        def _():
            pass_on(c - 1)

        when(0, more_queries)
        when(2, finish)
        when(0, attend)

        @pl.when((c > 1) & (c <= chunks))
        def _():
            pass_on(c - 1)

        when(0, terms)
        when(4, forward, spread)
        when(5, arrive, spread)

    lax.fori_loop(0, chunks + 2, turn, None)
    for c in (chunks - 2, chunks - 1):
        for kind in (OB, OA, RA, LB, RB, LA):
            remote(kind, c).wait_send()
        for b in range(2):
            local(c, b, False).wait()
    for c in (spread - 2, spread - 1):
        for kind in (FWR, FWL):
            remote(kind, c).wait_send()


def layer(x, gain, freq, wq, wk, wv, wo, n, axis):
    rows, d = x.shape
    wide, kv = wq.shape[1], wk.shape[1] // HEAD
    g = wide // HEAD // kv
    half = d // n // 2
    cols = g * ROWS
    vmem, hbm = pl.BlockSpec(memory_space=pltpu.VMEM), pl.BlockSpec(memory_space=pl.ANY)
    return pl.pallas_call(
        functools.partial(_kernel, n=n, axis=axis),
        in_specs=[vmem, vmem] + [hbm] * 5,
        out_specs=[hbm] * 3,
        out_shape=[jax.ShapeDtypeStruct((rows, d), BF16)] + [jax.ShapeDtypeStruct((LAST * ROWS, half), BF16)] * 2,
        scratch_shapes=[
            pltpu.VMEM(wq.shape, BF16),
            pltpu.VMEM((d, 2 * kv * HEAD), BF16),
            pltpu.VMEM(wo.shape, BF16),
            pltpu.VMEM((1, d), F32),
            pltpu.VMEM((ROWS, d), BF16),
            pltpu.VMEM((ROWS, d), BF16),
            pltpu.VMEM((ROWS, d // n), BF16),
            pltpu.VMEM((ROWS, HEAD), F32),
            pltpu.VMEM((ROWS, HEAD), F32),
            pltpu.VMEM((kv, cols, HEAD), BF16),
            pltpu.VMEM((rows, kv * HEAD), BF16),
            pltpu.VMEM((kv, HEAD + 16, rows), BF16),
            pltpu.VMEM((kv, cols), F32),
            pltpu.VMEM((kv, HEAD + 16, cols), F32),
            pltpu.VMEM((ROWS, wide), BF16),
            pltpu.VMEM((2, ROWS, half), F32),
            pltpu.VMEM((2, 2, ROWS, half), F32),
            pltpu.VMEM((2, 4, ROWS, half), BF16),
            pltpu.VMEM((2, 2, ROWS, half), BF16),
            pltpu.VMEM((2, 2, ROWS, half), BF16),
            pltpu.VMEM((2, 2, ROWS, half), BF16),
            pltpu.VMEM((4, 4, ROWS, half), BF16),
            pltpu.SemaphoreType.DMA((wide // 256 + 10,)),
            pltpu.SemaphoreType.DMA,
            pltpu.SemaphoreType.DMA((2, 2)),
            pltpu.SemaphoreType.DMA((12, 2)),
            pltpu.SemaphoreType.DMA((12, 4)),
        ],
        compiler_params=pltpu.CompilerParams(vmem_limit_bytes=VMEM, collective_id=0, has_side_effects=True),
        cost_estimate=pl.CostEstimate(
            flops=2 * rows * d * (2 * wide + 2 * kv * HEAD) + 2 * rows * rows * wide, transcendentals=rows * rows * wide // HEAD // 2,
            bytes_accessed=2 * (2 * d * wide + 2 * d * kv * HEAD + 2 * rows * d)),
        name="layer",
    )(freq, gain, x, wq, wk, wv, wo)


def _move(pairs, sem):
    copies = [pltpu.make_async_copy(a, b, sem.at[t]) for t, (a, b) in enumerate(pairs)]
    for copy in copies:
        copy.start()
    for copy in copies:
        copy.wait()


def _settle(from_ref, to_ref, sem, *, end):
    size = end // sem.shape[0]
    _move([(from_ref.at[pl.ds(t * size, size), :], to_ref.at[pl.ds(t * size, size), :]) for t in range(sem.shape[0])], sem)


def _place(*refs, n, axis, ahead):
    blocks, (to_ref, sem) = refs[: 2 * len(ahead)], refs[-2:]
    rows, half = blocks[0].shape
    owners = [lax.rem(lax.axis_index(axis) + t, n) for t in ahead]
    at = [pl.ds(pl.multiple_of((2 * owner + b) * half, 128), half) for owner in owners for b in range(2)]
    row = pl.ds(to_ref.shape[0] - rows, rows)
    _move([(block, to_ref.at[row, t]) for block, t in zip(blocks, at)], sem)


def into(kernel, shape, given, y, copies, name):
    hbm = pl.BlockSpec(memory_space=pl.ANY)
    size = sum(t.size for t in given)
    return pl.pallas_call(
        kernel,
        in_specs=[hbm] * (len(given) + (y is not None)),
        out_specs=hbm,
        out_shape=jax.ShapeDtypeStruct(shape, BF16),
        input_output_aliases={} if y is None else {len(given): 0},
        scratch_shapes=[pltpu.SemaphoreType.DMA((copies,))],
        compiler_params=pltpu.CompilerParams(vmem_limit_bytes=2**20),
        cost_estimate=pl.CostEstimate(flops=400 * size, transcendentals=0, bytes_accessed=4 * size),
        name=name,
    )(*given, *([] if y is None else [y]))


def solution(mesh):
    n = mesh.shape["tp"]
    right = lambda t: lax.ppermute(t, "tp", [(i, (i + 1) % n) for i in range(n)])
    left = lambda t: lax.ppermute(t, "tp", [(i, (i - 1) % n) for i in range(n)])

    def step(x, gain, wq, wk, wv, wo):
        half = HEAD // 2
        freq = np.float32(THETA) ** (-np.arange(half, dtype=np.float32) / np.float32(half))
        freq = jnp.asarray(np.concatenate([freq, freq]).reshape(1, HEAD))
        rows, d = x.shape
        t, fa, fb = layer(x, gain.reshape(-1, 128), freq, wq, wk, wv, wo, n, "tp")
        l_b, r_a = right(fb), left(fa)
        l_a, r_b = right(fa), left(fb)
        y = into(functools.partial(_settle, end=rows - LAST * ROWS), x.shape, [t], None, rows // ROWS - LAST, "settle")
        l_b, r_a, y = lax.optimization_barrier((l_b, r_a, y))
        o_b, o_a = right(l_b), left(r_a)
        place = lambda ahead, blocks, y: into(functools.partial(_place, n=n, axis="tp", ahead=ahead), x.shape, blocks, y, len(blocks), "place")
        y = place((0, 1, n - 1), [fa, fb, r_a, r_b, l_a, l_b], y)
        return place((2,), [o_a, o_b], y)

    tokens, columns = P("dp", None), P(None, "tp")
    return jax.shard_map(
        step,
        mesh=mesh,
        in_specs=(tokens, P(None), columns, columns, columns, P("tp", None)),
        out_specs=tokens,
        check_vma=False,
    )
```

```python
import functools

import jax
import jax.numpy as jnp
import numpy as np
from jax import lax
from jax.experimental import pallas as pl
from jax.experimental.pallas import tpu as pltpu
from jax.sharding import PartitionSpec as P

HEAD = 128
THETA = 10000
NEG = float(np.finfo(np.float32).min)
LOG2E = 1.4426950408889634
VMEM = 67_000_000
ROWS = 128
KEYS = 256
AHEAD = 3
LAST = 3
F32, BF16 = jnp.float32, jnp.bfloat16
OB, OA, RA, LB, RB, LA, YBR, YAR, YAL, YBL, FWR, FWL = range(12)


def _dot(a, b, ca, cb):
    return lax.dot_general(a, b, (((ca,), (cb,)), ((), ())), preferred_element_type=F32)


def _kernel(freq_ref, gain_ref, x_hbm, wq_hbm, wk_hbm, wv_hbm, wo_hbm, y_hbm, fa_hbm, fb_hbm,
            wq, wkv, wo, gain_s, x_s, h_s, xown_s, cos_s, sin_s, q_s, k_s, vt_s, top_s, mix_s, seen_s,
            mid_s, own_s, term_s, pass_s, fin_s, got_s, far_s,
            w_sem, x_sem, y_sem, send_sem, recv_sem, *, n, axis):
    rows, d = x_hbm.shape
    chunks = rows // ROWS
    spread = chunks - LAST
    wide = wq.shape[1]
    kv = wk_hbm.shape[1] // HEAD
    g = wide // HEAD // kv
    part, half = d // n, d // n // 2
    cols = g * ROWS
    strip = cols // 2
    e = HEAD**-0.5 * LOG2E
    i = lax.axis_index(axis)
    r, l, o = lax.rem(i + 1, n), lax.rem(i + n - 1, n), lax.rem(i + 2, n)

    def column(owner, b):
        return pl.ds(pl.multiple_of(owner * part + b * half, 128), half)

    def columns(owner):
        return pl.ds(pl.multiple_of(owner * part, 128), part)

    def row(c):
        return pl.ds(pl.multiple_of(c * ROWS, ROWS), ROWS)

    def remote(kind, c):
        s2, s4 = lax.rem(c, 2), lax.rem(c, 4)
        to = r if kind in (OB, RA, RB, YBR, YAR, FWR) else l
        if kind in (OB, OA):
            src, dst = term_s.at[s2, kind], got_s.at[s2, kind]
        elif kind in (RA, LB):
            src, dst = term_s.at[s2, kind], far_s.at[s4, kind - RA]
        elif kind in (RB, LA):
            src, dst = pass_s.at[s2, kind - RB], far_s.at[s4, kind - RA]
        elif kind in (YBR, YBL):
            src, dst = fin_s.at[s2, 1], y_hbm.at[row(c), column(i, 1)]
        elif kind in (YAR, YAL):
            src, dst = fin_s.at[s2, 0], y_hbm.at[row(c), column(i, 0)]
        elif kind == FWR:
            src = dst = y_hbm.at[row(c), column(l, 1)]
        else:
            src = dst = y_hbm.at[row(c), column(r, 0)]
        return pltpu.make_async_remote_copy(
            src_ref=src, dst_ref=dst, send_sem=send_sem.at[kind, s2], recv_sem=recv_sem.at[kind, s4],
            device_id={axis: to}, device_id_type=pl.DeviceIdType.MESH,
        )

    def local(c, b, here=True):
        to = y_hbm.at[row(c), column(i, b)] if here else (fa_hbm, fb_hbm)[b].at[row(c - spread), :]
        s2 = lax.rem(c, 2)
        return pltpu.make_async_copy(fin_s.at[s2, b], to, y_sem.at[b, s2])

    def chunk_in(c):
        return pltpu.make_async_copy(x_hbm.at[row(c), :], x_s, x_sem)

    tile = 512
    q_tiles = [pltpu.make_async_copy(wq_hbm.at[:, pl.ds(t * tile, tile)], wq.at[:, pl.ds(t * tile, tile)], w_sem.at[t]) for t in range(wide // tile)]
    k_in = pltpu.make_async_copy(wk_hbm, wkv.at[:, : kv * HEAD], w_sem.at[len(q_tiles)])
    v_in = pltpu.make_async_copy(wv_hbm, wkv.at[:, kv * HEAD :], w_sem.at[len(q_tiles) + 1])
    owners = (o, r, l, i)
    o_tiles = [pltpu.make_async_copy(wo_hbm.at[:, columns(t)], wo.at[:, columns(t)], w_sem.at[len(q_tiles) + 2 + p]) for p, t in enumerate(owners)]

    chunk_in(0).start()
    loads = [k_in, v_in, *q_tiles, *o_tiles]
    for copy in loads[:AHEAD]:
        copy.start()
    barrier = pltpu.get_barrier_semaphore()
    for to in (l, r):
        pl.semaphore_signal(barrier, inc=1, device_id={axis: to}, device_id_type=pl.DeviceIdType.MESH)

    for t in range(d // 128):
        gain_s[:, t * 128 : (t + 1) * 128] = gain_ref[t : t + 1, :].astype(F32)
    k_s[...] = jnp.zeros(k_s.shape, BF16)
    for m in range(kv):
        vt_s[m, :HEAD, :] = jnp.zeros((HEAD, rows), BF16)
        vt_s[m, HEAD:, :] = jnp.ones((vt_s.shape[1] - HEAD, rows), BF16)
    pl.semaphore_wait(barrier, 2)

    def turned(t):
        t = t.astype(BF16).astype(F32)
        return (t * cos_s[...] + pltpu.roll(t, HEAD // 2, 1) * sin_s[...]).astype(BF16)

    def first(c, number):
        @pl.when(c == 0)
        def _():
            loads[number].wait()
            if number + AHEAD < len(loads):
                loads[number + AHEAD].start()

    def project(c):
        chunk_in(c).wait()

        def norm(t, _):
            at = pl.ds(pl.multiple_of(t * 16, 16), 16)
            w = x_s[at, :].astype(F32)
            scale = lax.rsqrt(jnp.mean(w * w, -1, keepdims=True) + 1e-6)
            h_s[at, :] = (w * scale * gain_s[...]).astype(BF16)

        lax.fori_loop(0, ROWS // 16, norm, None)
        xown_s[...] = x_s[:, columns(i)]

        @pl.when((c > 0) & (c + 1 < chunks))
        def _():
            chunk_in(c + 1).start()

        place = lax.broadcasted_iota(jnp.int32, (ROWS, HEAD), 0) + c * ROWS
        angle = place.astype(F32) * freq_ref[...]
        sign = jnp.where(lax.broadcasted_iota(jnp.int32, (ROWS, HEAD), 1) < HEAD // 2, -1.0, 1.0)
        cos_s[...] = jnp.cos(angle)
        sin_s[...] = jnp.sin(angle) * sign

        first(c, 0)
        first(c, 1)
        t = _dot(h_s[...], wkv[...], 1, 0)
        for m in range(kv):
            k_s[row(c), m * HEAD : (m + 1) * HEAD] = turned(t[:, m * HEAD : (m + 1) * HEAD])
            vt_s[m, :HEAD, row(c)] = t[:, (kv + m) * HEAD : (kv + m + 1) * HEAD].T.astype(BF16)
        queries(c, 0)

    def queries(c, p):
        first(c, 2 + p)
        t = _dot(h_s[...], wq[:, p * tile : (p + 1) * tile], 1, 0)
        for m in range(tile // HEAD):
            head = p * (tile // HEAD) + m
            q_s[head // g, head % g * ROWS : (head % g + 1) * ROWS, :] = turned(t[:, m * HEAD : (m + 1) * HEAD])

    def more_queries(c):
        for p in range(1, len(q_tiles)):
            queries(c, p)

    def attend(c):
        pieces = [(m, at) for m in range(kv) for at in range(0, cols, strip)]
        top_s[...] = jnp.full(top_s.shape, NEG, F32)
        mix_s[...] = jnp.zeros(mix_s.shape, F32)

        def block(j, masked, keys=KEYS):
            here = pl.ds(pl.multiple_of(j * KEYS, KEYS), keys)
            scores = [_dot(k_s[here, m * HEAD : (m + 1) * HEAD], q_s[m, at : at + strip, :], 1, 1) for m, at in pieces]
            if masked:
                query = lax.rem(lax.broadcasted_iota(jnp.int32, (keys, strip), 1), ROWS) + c * ROWS
                ok = query >= lax.broadcasted_iota(jnp.int32, (keys, strip), 0) + j * KEYS
            weights, keeps = [], []
            for (m, at), s in zip(pieces, scores):
                if masked:
                    s = jnp.where(ok, s, NEG)
                old = top_s[m : m + 1, at : at + strip]
                top = jnp.maximum(old, s.max(axis=0, keepdims=True))
                top_s[m : m + 1, at : at + strip] = top
                weights.append(jnp.exp2((s - top) * e).astype(BF16))
                keeps.append(jnp.exp2((old - top) * e))
            for (m, at), p, keep in zip(pieces, weights, keeps):
                mix_s[m, :, at : at + strip] = mix_s[m, :, at : at + strip] * keep + _dot(vt_s[m, :, here], p, 1, 0)

        whole = lax.div(c * ROWS, KEYS)
        lax.fori_loop(0, whole, lambda j, _: block(j, False), None)
        for t in range(KEYS // ROWS):

            @pl.when(lax.rem(c, KEYS // ROWS) == t)
            def _(t=t):
                block(whole, True, (t + 1) * ROWS)

        for m in range(kv):
            out = (mix_s[m, :HEAD, :] * (1 / mix_s[m, HEAD : HEAD + 1, :])).T.astype(BF16)
            for h in range(g):
                at = (m * g + h) * HEAD
                seen_s[:, at : at + HEAD] = out[h * ROWS : (h + 1) * ROWS, :]

    def terms(c):
        s2 = lax.rem(c, 2)

        def product(p):
            first(c, 2 + len(q_tiles) + p)
            return _dot(seen_s[...], wo[:, columns(owners[p])], 1, 0)

        @pl.when(c >= 2)
        def _():
            for kind in (OB, OA, RA, LB):
                remote(kind, c - 2).wait_send()

        t = product(0)
        term_s[s2, OB], term_s[s2, OA] = t[:, half:].astype(BF16), t[:, :half].astype(BF16)
        remote(OB, c).start()
        remote(OA, c).start()

        @pl.when(c == 0)
        def _():
            chunk_in(1).start()

        t = product(1)
        term_s[s2, RA], mid_s[0] = t[:, :half].astype(BF16), t[:, half:]
        remote(RA, c).start()
        t = product(2)
        term_s[s2, LB], mid_s[1] = t[:, half:].astype(BF16), t[:, :half]
        remote(LB, c).start()
        t = product(3)
        for b in range(2):
            own_s[s2, b] = xown_s[:, b * half : (b + 1) * half].astype(F32) + t[:, b * half : (b + 1) * half]

    def pass_on(c):
        s2 = lax.rem(c, 2)

        @pl.when(c >= 2)
        def _():
            for kind in (RB, LA):
                remote(kind, c - 2).wait_send()

        for kind in (OB, OA):
            remote(kind, c).wait_recv()
            pass_s[s2, kind] = (mid_s[kind] + got_s[s2, kind].astype(F32)).astype(BF16)
        for kind in (RB, LA):
            remote(kind, c).start()

    def finish(c):
        s2, s4 = lax.rem(c, 2), lax.rem(c, 4)

        @pl.when((c >= 2) & (c < spread + 2))
        def _():
            for kind in (YBR, YAR, YAL, YBL):
                remote(kind, c - 2).wait_send()
            for b in range(2):
                local(c - 2, b).wait()

        @pl.when(c >= spread + 2)
        def _():
            for b in range(2):
                local(c - 2, b, False).wait()

        for kind in (RA, LB, RB, LA):
            remote(kind, c).wait_recv()
        fin_s[s2, 1] = (own_s[s2, 1] + far_s[s4, LB - RA].astype(F32) + far_s[s4, RB - RA].astype(F32)).astype(BF16)
        fin_s[s2, 0] = (own_s[s2, 0] + far_s[s4, RA - RA].astype(F32) + far_s[s4, LA - RA].astype(F32)).astype(BF16)
        @pl.when(c < spread)
        def _():
            for kind in (YBR, YAL, YAR, YBL):
                remote(kind, c).start()
            for b in range(2):
                local(c, b).start()

        @pl.when(c >= spread)
        def _():
            for b in range(2):
                local(c, b, False).start()

    def forward(c):
        @pl.when(c >= 2)
        def _():
            for kind in (FWR, FWL):
                remote(kind, c - 2).wait_send()

        for kind, after in ((FWR, YBR), (FWL, YAL)):
            remote(after, c).wait_recv()
            remote(kind, c).start()
        for kind in (YAR, YBL):
            remote(kind, c).wait_recv()

    def arrive(c):
        for kind in (FWR, FWL):
            remote(kind, c).wait_recv()

    def turn(c, _):
        def when(lag, do, end=chunks):
            @pl.when((c >= lag) & (c < end + lag))
            def _():
                do(c - lag)

        when(0, project)

        @pl.when(c == 1)
        def _():
            pass_on(c - 1)

        when(0, more_queries)
        when(2, finish)
        when(0, attend)

        @pl.when((c > 1) & (c <= chunks))
        def _():
            pass_on(c - 1)

        when(0, terms)
        when(4, forward, spread)
        when(5, arrive, spread)

    lax.fori_loop(0, chunks + 2, turn, None)
    for c in (chunks - 2, chunks - 1):
        for kind in (OB, OA, RA, LB, RB, LA):
            remote(kind, c).wait_send()
        for b in range(2):
            local(c, b, False).wait()
    for c in (spread - 2, spread - 1):
        for kind in (FWR, FWL):
            remote(kind, c).wait_send()


def layer(x, gain, freq, wq, wk, wv, wo, n, axis):
    rows, d = x.shape
    wide, kv = wq.shape[1], wk.shape[1] // HEAD
    g = wide // HEAD // kv
    half = d // n // 2
    cols = g * ROWS
    vmem, hbm = pl.BlockSpec(memory_space=pltpu.VMEM), pl.BlockSpec(memory_space=pl.ANY)
    return pl.pallas_call(
        functools.partial(_kernel, n=n, axis=axis),
        in_specs=[vmem, vmem] + [hbm] * 5,
        out_specs=[hbm] * 3,
        out_shape=[jax.ShapeDtypeStruct((rows, d), BF16)] + [jax.ShapeDtypeStruct((LAST * ROWS, half), BF16)] * 2,
        scratch_shapes=[
            pltpu.VMEM(wq.shape, BF16),
            pltpu.VMEM((d, 2 * kv * HEAD), BF16),
            pltpu.VMEM(wo.shape, BF16),
            pltpu.VMEM((1, d), F32),
            pltpu.VMEM((ROWS, d), BF16),
            pltpu.VMEM((ROWS, d), BF16),
            pltpu.VMEM((ROWS, d // n), BF16),
            pltpu.VMEM((ROWS, HEAD), F32),
            pltpu.VMEM((ROWS, HEAD), F32),
            pltpu.VMEM((kv, cols, HEAD), BF16),
            pltpu.VMEM((rows, kv * HEAD), BF16),
            pltpu.VMEM((kv, HEAD + 16, rows), BF16),
            pltpu.VMEM((kv, cols), F32),
            pltpu.VMEM((kv, HEAD + 16, cols), F32),
            pltpu.VMEM((ROWS, wide), BF16),
            pltpu.VMEM((2, ROWS, half), F32),
            pltpu.VMEM((2, 2, ROWS, half), F32),
            pltpu.VMEM((2, 4, ROWS, half), BF16),
            pltpu.VMEM((2, 2, ROWS, half), BF16),
            pltpu.VMEM((2, 2, ROWS, half), BF16),
            pltpu.VMEM((2, 2, ROWS, half), BF16),
            pltpu.VMEM((4, 4, ROWS, half), BF16),
            pltpu.SemaphoreType.DMA((wide // 256 + 10,)),
            pltpu.SemaphoreType.DMA,
            pltpu.SemaphoreType.DMA((2, 2)),
            pltpu.SemaphoreType.DMA((12, 2)),
            pltpu.SemaphoreType.DMA((12, 4)),
        ],
        compiler_params=pltpu.CompilerParams(vmem_limit_bytes=VMEM, collective_id=0, has_side_effects=True),
        cost_estimate=pl.CostEstimate(
            flops=2 * rows * d * (2 * wide + 2 * kv * HEAD) + 2 * rows * rows * wide, transcendentals=rows * rows * wide // HEAD // 2,
            bytes_accessed=2 * (2 * d * wide + 2 * d * kv * HEAD + 2 * rows * d)),
        name="layer",
    )(freq, gain, x, wq, wk, wv, wo)


def _move(pairs, sem):
    copies = [pltpu.make_async_copy(a, b, sem.at[t]) for t, (a, b) in enumerate(pairs)]
    for copy in copies:
        copy.start()
    for copy in copies:
        copy.wait()


def _settle(from_ref, to_ref, sem, *, end):
    size = end // sem.shape[0]
    _move([(from_ref.at[pl.ds(t * size, size), :], to_ref.at[pl.ds(t * size, size), :]) for t in range(sem.shape[0])], sem)


def _place(*refs, n, axis, ahead):
    blocks, (to_ref, sem) = refs[: 2 * len(ahead)], refs[-2:]
    rows, half = blocks[0].shape
    owners = [lax.rem(lax.axis_index(axis) + t, n) for t in ahead]
    at = [pl.ds(pl.multiple_of((2 * owner + b) * half, 128), half) for owner in owners for b in range(2)]
    row = pl.ds(to_ref.shape[0] - rows, rows)
    _move([(block, to_ref.at[row, t]) for block, t in zip(blocks, at)], sem)


def into(kernel, shape, given, y, copies, name):
    hbm = pl.BlockSpec(memory_space=pl.ANY)
    size = sum(t.size for t in given)
    return pl.pallas_call(
        kernel,
        in_specs=[hbm] * (len(given) + (y is not None)),
        out_specs=hbm,
        out_shape=jax.ShapeDtypeStruct(shape, BF16),
        input_output_aliases={} if y is None else {len(given): 0},
        scratch_shapes=[pltpu.SemaphoreType.DMA((copies,))],
        compiler_params=pltpu.CompilerParams(vmem_limit_bytes=2**20),
        cost_estimate=pl.CostEstimate(flops=400 * size, transcendentals=0, bytes_accessed=4 * size),
        name=name,
    )(*given, *([] if y is None else [y]))


def solution(mesh):
    n = mesh.shape["tp"]
    right = lambda t: lax.ppermute(t, "tp", [(i, (i + 1) % n) for i in range(n)])
    left = lambda t: lax.ppermute(t, "tp", [(i, (i - 1) % n) for i in range(n)])

    def step(x, gain, wq, wk, wv, wo):
        half = HEAD // 2
        freq = np.float32(THETA) ** (-np.arange(half, dtype=np.float32) / np.float32(half))
        freq = jnp.asarray(np.concatenate([freq, freq]).reshape(1, HEAD))
        rows, d = x.shape
        t, fa, fb = layer(x, gain.reshape(-1, 128), freq, wq, wk, wv, wo, n, "tp")
        l_b, r_a = right(fb), left(fa)
        l_a, r_b = right(fa), left(fb)
        y = into(functools.partial(_settle, end=rows - LAST * ROWS), x.shape, [t], None, rows // ROWS - LAST, "settle")
        l_b, r_a, y = lax.optimization_barrier((l_b, r_a, y))
        o_b, o_a = right(l_b), left(r_a)
        place = lambda ahead, blocks, y: into(functools.partial(_place, n=n, axis="tp", ahead=ahead), x.shape, blocks, y, len(blocks), "place")
        y = place((0, 1, n - 1), [fa, fb, r_a, r_b, l_a, l_b], y)
        return place((2,), [o_a, o_b], y)

    tokens, columns = P("dp", None), P(None, "tp")
    return jax.shard_map(
        step,
        mesh=mesh,
        in_specs=(tokens, P(None), columns, columns, columns, P("tp", None)),
        out_specs=tokens,
        check_vma=False,
    )
```
